128 devices in a mesh: clip: 4 (over y_hi, core), frame: 32 (over z, x, y_lo).
Axes of the slice: x: 4, y: 4 (y_hi: 2, y_lo: 2; y = y_hi * 2 + y_lo), z: 4, core: 2. Of those that a mesh axis runs over, the one named last changes fastest.
Arguments:
- video: bfloat16 [512, 512, 512], P(('clip', 'frame')), parts along dimension 0, may hold values from -6 to 6
- timestep: int32 [4], P('clip'), parts along dimension 0, may hold values from 0 to 999
- cond_weight: bfloat16 [128, 2048], replicated, may hold values from -0.5 to 0.5
- spatial_gain: float32 [512], replicated, may hold values from 0.25 to 1.75
- spatial_qkv: bfloat16 [512, 1536], replicated, may hold values from -0.25 to 0.25
- spatial_out: bfloat16 [512, 512], replicated, may hold values from -0.25 to 0.25
- temporal_gain: float32 [512], replicated, may hold values from 0.25 to 1.75
- temporal_qkv: bfloat16 [512, 1536], replicated, may hold values from -0.25 to 0.25
- temporal_out: bfloat16 [512, 512], replicated, may hold values from -0.25 to 0.25
- merge_weight: bfloat16 [4096, 1024], replicated, may hold values from -0.09375 to 0.09375
- coarse_gain: float32 [1024], replicated, may hold values from 0.25 to 1.75
- coarse_qkv: bfloat16 [1024, 3072], replicated, may hold values from -0.1875 to 0.1875
- coarse_out: bfloat16 [1024, 1024], replicated, may hold values from -0.1875 to 0.1875
- up_weight: bfloat16 [1024, 512], replicated, may hold values from -0.1875 to 0.1875
Outputs:
- denoised: bfloat16 [512, 512, 512], P(('clip', 'frame')), parts along dimension 0
The draws below stay inside these ranges and needn't reach their ends.
There are 4 independent parts, one for each index of `clip`. The reference program is written for one: setup_inputs(seed, part) draws one part's arguments, and reference() takes and returns one part's arrays. A program takes and returns all parts, laid end to end along the dimension named above; an argument that names none is the same for every part. Nothing has to cross between parts.
All inputs are finite; a program needn't handle non-finite values.
Results may differ from the reference program's by a relative error of at most 0.015.
Values may be sent and summed in bfloat16 or wider, within the bound.
A program may use at most 192 MiB of HBM per device.

```python
import math
import jax
import jax.numpy as jnp
from jax import lax

D = 512
DC = 1024
HEAD = 64
FREQ = 64
TOK = 512
FRAMES = 128
BLK = 128


def levels(own_key, extent, cuts, low, largest):
    def one(dim, parts):
        draws = jax.random.uniform(jax.random.fold_in(jax.random.fold_in(own_key, 6), dim), (parts,), jnp.float32, low / len(cuts), largest / len(cuts))
        return jnp.repeat(jnp.exp(draws), extent[dim] // parts).reshape((-1,) + (1,) * (len(extent) - dim - 1))

    factor_of = one(*cuts[0])
    for cut in cuts[1:]:
        factor_of = factor_of * one(*cut)
    return factor_of


def centred(stream_key, extent, width, limit, shards=(), kind=jnp.bfloat16):
    factor_of = levels(stream_key, extent, shards, -0.22, 0.18) if shards else 1.0
    array = jax.random.normal(stream_key, extent, jnp.float32) * width * factor_of
    return jnp.minimum(jnp.maximum(array, -limit), limit).astype(kind)


def setup_inputs(seed: int = 0, part: int = 0) -> dict:
    seeds = jax.random.split(jax.random.key(seed), 15)
    part_splits = jax.random.split(jax.random.fold_in(seeds[14], part), 15)
    return {
        "video": centred(part_splits[0], (FRAMES, TOK, D), 1.0, 6.0, ((0, 32),)),
        "timestep": jax.random.randint(part_splits[1], (1,), 0, 1000).astype(jnp.int32),
        "cond_weight": centred(seeds[2], (2 * FREQ, 4 * D), (2 * FREQ) ** -0.5, 0.5),
        "spatial_gain": jnp.clip(1.0 + 0.15 * jax.random.normal(seeds[3], (D,), jnp.float32), 0.25, 1.75),
        "spatial_qkv": centred(seeds[4], (D, 3 * D), D ** -0.5, 0.25),
        "spatial_out": centred(seeds[5], (D, D), D ** -0.5, 0.25),
        "temporal_gain": jnp.clip(1.0 + 0.15 * jax.random.normal(seeds[6], (D,), jnp.float32), 0.25, 1.75),
        "temporal_qkv": centred(seeds[7], (D, 3 * D), D ** -0.5, 0.25),
        "temporal_out": centred(seeds[8], (D, D), D ** -0.5, 0.25),
        "merge_weight": centred(seeds[9], (8 * D, DC), (8 * D) ** -0.5, 0.09375),
        "coarse_gain": jnp.clip(1.0 + 0.15 * jax.random.normal(seeds[10], (DC,), jnp.float32), 0.25, 1.75),
        "coarse_qkv": centred(seeds[11], (DC, 3 * DC), DC ** -0.5, 0.1875),
        "coarse_out": centred(seeds[12], (DC, DC), DC ** -0.5, 0.1875),
        "up_weight": centred(seeds[13], (DC, D), DC ** -0.5, 0.1875),
    }


def modulation_of(timestep, cond_weight):
    counter = jnp.arange(FREQ, dtype=jnp.float32)
    frequency = jnp.exp(counter * (-math.log(10000.0) / FREQ))
    angles = timestep.astype(jnp.float32)[0] * frequency
    embedding = jnp.concatenate([jnp.sin(angles), jnp.cos(angles)])
    return jnp.dot(embedding[None, :], cond_weight.astype(jnp.float32), precision=lax.Precision.HIGHEST)[0]

def attention_block(inputs, gain_vec, scale_mod, shift_mod, w_qkv, w_out, head_count):
    length, batched, features = inputs.shape
    widened = inputs.astype(jnp.float32)
    mean_square = lax.optimization_barrier(jnp.mean(widened * widened, axis=-1, keepdims=True))
    normed = (widened * lax.rsqrt(mean_square + 1e-06) * gain_vec * (1.0 + scale_mod) + shift_mod).astype(jnp.bfloat16)
    projected = jnp.dot(normed.reshape(length * batched, features), w_qkv, preferred_element_type=jnp.float32)
    projected = projected.astype(jnp.bfloat16).reshape(length, batched, 3, head_count, features // head_count)
    queries = projected[:, :, 0].astype(jnp.float32)
    keys = projected[:, :, 1].astype(jnp.float32)
    values = projected[:, :, 2].astype(jnp.float32)
    scores = jnp.einsum('snhe,tnhe->nhst', queries, keys) * (1.0 / math.sqrt(features // head_count))
    probs = jax.nn.softmax(scores, axis=-1).astype(jnp.bfloat16)
    mixed = jnp.einsum('nhst,tnhe->snhe', probs.astype(jnp.float32), values)
    mixed = mixed.astype(jnp.bfloat16).reshape(length * batched, features)
    update = jnp.dot(mixed, w_out, preferred_element_type=jnp.float32).reshape(length, batched, features)
    return (widened + update).astype(jnp.bfloat16)

def merge_frames(fine_tokens, merge_weight):
    frames_here, blocks, quads, features = fine_tokens.shape
    paired = fine_tokens.reshape(frames_here // 2, 2, blocks, quads, features).transpose(0, 2, 1, 3, 4)
    paired = paired.reshape(frames_here // 2 * blocks, 2 * quads * features)
    merged = jnp.dot(paired, merge_weight, preferred_element_type=jnp.float32).astype(jnp.bfloat16)
    return merged.reshape(frames_here // 2, blocks, merge_weight.shape[1])

def combine_levels(fine_tokens, coarse_tokens, up_weight):
    frames_here, blocks, quads, features = fine_tokens.shape
    upsampled = jnp.dot(coarse_tokens.reshape(-1, coarse_tokens.shape[2]), up_weight, preferred_element_type=jnp.float32)
    upsampled = upsampled.reshape(frames_here // 2, 1, blocks, 1, features)
    result = fine_tokens.astype(jnp.float32).reshape(frames_here // 2, 2, blocks, quads, features) + upsampled
    return result.astype(jnp.bfloat16).reshape(fine_tokens.shape)

def reference(video, timestep, cond_weight, spatial_gain, spatial_qkv, spatial_out, temporal_gain, temporal_qkv, temporal_out, merge_weight, coarse_gain, coarse_qkv, coarse_out, up_weight):
    modulation = modulation_of(timestep, cond_weight)
    scale_s, shift_s, scale_t, shift_t = [modulation[i * D:(i + 1) * D] for i in range(4)]

    def spatial(frame_rows):
        return attention_block(frame_rows[:, None, :], spatial_gain, scale_s, shift_s, spatial_qkv, spatial_out, D // HEAD)[:, 0, :]
    fine1 = lax.map(spatial, video)
    grouped = jnp.moveaxis(fine1.reshape(FRAMES, BLK, 4, D), 1, 0)

    def temporal(cell_rows):
        return attention_block(cell_rows, temporal_gain, scale_t, shift_t, temporal_qkv, temporal_out, D // HEAD)
    fine2 = jnp.moveaxis(lax.map(temporal, grouped), 0, 1)
    coarse0 = merge_frames(fine2, merge_weight)
    coarse1 = attention_block(coarse0, coarse_gain, 0.0, 0.0, coarse_qkv, coarse_out, DC // HEAD)
    return combine_levels(fine2, coarse1, up_weight).reshape(FRAMES, TOK, D)
```

```python
import math

import jax
import jax.numpy as jnp
from jax import lax
from jax.experimental import pallas as pl
from jax.experimental.pallas import tpu as pltpu
from jax.sharding import PartitionSpec as P

D = 512
DC = 1024
HEAD = 64
FREQ = 64
GROUP = 32
MESH = pl.DeviceIdType.MESH
F32 = jnp.float32
BF16 = jnp.bfloat16
QSCALE = math.log2(math.e) / math.sqrt(HEAD)

OFFSETS = sorted(
    [(a, b, d) for a in range(4) for b in range(4) for d in range(2) if (a, b, d) != (0, 0, 0)],
    key=lambda o: -(min(o[0], 4 - o[0]) + min(o[1], 4 - o[1]) + o[2]),
)


def dot(a, b):
    return jnp.dot(a, b, preferred_element_type=F32)


def dot_t(a, b):
    return lax.dot_general(a, b, (((1,), (1,)), ((), ())), preferred_element_type=F32)


def onehot(rows, columns, column_of):
    r = lax.broadcasted_iota(jnp.int32, (rows, columns), 0)
    c = lax.broadcasted_iota(jnp.int32, (rows, columns), 1)
    return jnp.where(c == column_of(r), 1.0, 0.0).astype(BF16)


def rms(x):
    return x * lax.rsqrt(jnp.mean(x * x, axis=-1, keepdims=True) + 1e-06)


def pair_attention(q2, kst, vst, ones, keys):
    s = dot_t(q2, kst)
    s_lo, s_hi = s[:, :keys], s[:, keys:]
    p_lo = jnp.exp2(s_lo - jnp.max(s_lo, axis=-1, keepdims=True)).astype(BF16)
    p_hi = jnp.exp2(s_hi - jnp.max(s_hi, axis=-1, keepdims=True)).astype(BF16)
    p = jnp.concatenate([p_lo, p_hi], axis=1)
    o = dot(p, jnp.concatenate([vst, ones], axis=1))
    return (o[:, :128] / o[:, 128:]).astype(BF16)


def kernel(
    video, emb, cond, sgain, sqkv, sout, tgain, tqkv, tout, merge, cgain, cqkv, cout, up,
    out,
    vid, wcond, wsq, wso, wtq, wto, wm, wcq, wco, wup,
    sq, skst, svst, ones_s, smix,
    sbuf1, recv1,
    perm, xt, tq, tkst, tvst, ones_t, tmix,
    sbuf2, cbuf, recv2,
    c0, cq, ck, cv, cmix, zs, zr,
    modv, lsem, vsem, osem, ss1, rs1, ss2, rs2, ss3, rs3,
):
    clip = lax.axis_index("clip")
    me = lax.axis_index("frame")
    z, x, y = me // 8, lax.rem(me // 2, 4), lax.rem(me, 2)

    def peer(o):
        return lax.rem(z + o[0], 4) * 8 + lax.rem(x + o[1], 4) * 2 + lax.rem(y + o[2], 2)

    barrier = pltpu.get_barrier_semaphore()
    for o in OFFSETS:
        pl.semaphore_signal(barrier, inc=1, device_id=(clip, peer(o)), device_id_type=MESH)

    weights = [
        (cond, wcond), (sqkv, wsq), (sout, wso), (tqkv, wtq), (tout, wto),
        (merge, wm), (cqkv, wcq), (cout, wco), (up, wup),
    ]
    wcopy = [pltpu.make_async_copy(a, b, lsem.at[i]) for i, (a, b) in enumerate(weights)]
    vcopy = [pltpu.make_async_copy(video.at[f], vid.at[f], vsem.at[f]) for f in range(4)]
    vcopy[0].start()
    for i in range(3):
        wcopy[i].start()
    for f in range(1, 4):
        vcopy[f].start()

    lane = lax.broadcasted_iota(jnp.int32, (1, 128), 1)
    lo = jnp.where(lane < HEAD, 1.0, 0.0).astype(F32)
    hi = 1.0 - lo
    ones_s[0:512, :] = jnp.broadcast_to(lo, (512, 128)).astype(BF16)
    ones_s[512:1024, :] = jnp.broadcast_to(hi, (512, 128)).astype(BF16)
    ones_t[0:128, :] = jnp.broadcast_to(lo, (128, 128)).astype(BF16)
    ones_t[128:256, :] = jnp.broadcast_to(hi, (128, 128)).astype(BF16)
    perm[0] = onehot(256, 256, lambda r: (r & 15) * 16 + (r >> 4))
    perm[1] = onehot(
        256, 256,
        lambda r: ((r & 3) * 4 + ((r >> 5) & 3)) * 16 + ((r >> 2) & 7) * 2 + (r >> 7),
    )
    perm[2] = onehot(256, 256, lambda r: (r & 63) * 4 + (r >> 6))

    wcopy[0].wait()
    modv[...] = jnp.sum(emb[...] * wcond[...].astype(F32), axis=0, keepdims=True)
    sg = sgain[...] * (1.0 + modv[:, 0:D])
    shs = modv[:, D : 2 * D]
    tg = tgain[...] * (1.0 + modv[:, 2 * D : 3 * D])
    sht = modv[:, 3 * D : 4 * D]

    wcopy[1].wait()
    wcopy[2].wait()
    for f in range(4):
        vcopy[f].wait()
    for i in range(3, 9):
        wcopy[i].start()
    pl.semaphore_wait(barrier, len(OFFSETS))

    def frame_step(f, carry):
        xf = vid[f].astype(F32)
        normed = (rms(xf) * sg + shs).astype(BF16)
        sq[...] = (dot(normed, wsq[:, 0:D]) * QSCALE).astype(BF16)
        for p in range(4):
            k2 = dot(normed, wsq[:, D + p * 128 : D + (p + 1) * 128])
            skst[p, 0:512] = (k2 * lo).astype(BF16)
            skst[p, 512:1024] = (k2 * hi).astype(BF16)
            v2 = dot(normed, wsq[:, 2 * D + p * 128 : 2 * D + (p + 1) * 128])
            svst[p, 0:512] = (v2 * lo).astype(BF16)
            svst[p, 512:1024] = (v2 * hi).astype(BF16)

        for p in range(4):
            def rows_step(i, c, p=p):
                rows = pl.ds(pl.multiple_of(i * 256, 256), 256)
                smix[rows, p * 128 : (p + 1) * 128] = pair_attention(
                    sq[rows, p * 128 : (p + 1) * 128], skst[p], svst[p], ones_s[...], 512
                )
                return c

            lax.fori_loop(0, 2, rows_step, 0)
        fine1 = (vid[f].astype(F32) + dot(smix[...], wso[...])).astype(BF16)
        sbuf1[f] = fine1
        own = pl.ds(pl.multiple_of(me * 16, 16), 16)
        recv1[me * 4 + f] = sbuf1[f, own, :]
        for o in OFFSETS:
            to = peer(o)
            pltpu.make_async_remote_copy(
                src_ref=sbuf1.at[f, pl.ds(pl.multiple_of(to * 16, 16), 16), :],
                dst_ref=recv1.at[me * 4 + f],
                send_sem=ss1,
                recv_sem=rs1,
                device_id=(clip, to),
                device_id_type=MESH,
            ).start()
        return carry

    lax.fori_loop(0, 4, frame_step, 0)

    wcopy[3].wait()
    wcopy[4].wait()
    pltpu.make_async_copy(recv1.at[pl.ds(0, 124)], recv1.at[pl.ds(0, 124)], rs1).wait()

    def group_step(g, carry):
        frames = pl.ds(pl.multiple_of(g * 16, 16), 16)
        xg = recv1[frames].reshape(256, D)
        yg = dot(perm[0], xg)
        xt[:, frames, :] = yg.astype(BF16).reshape(16, 16, D)
        normed = (rms(yg) * tg + sht).astype(BF16)
        tq[:, frames, :] = (dot(normed, wtq[:, 0:D]) * QSCALE).astype(BF16).reshape(16, 16, D)
        high = pl.ds(pl.multiple_of(128 + g * 16, 16), 16)
        for p in range(4):
            k2 = dot(normed, wtq[:, D + p * 128 : D + (p + 1) * 128])
            tkst[:, p, frames, :] = (k2 * lo).astype(BF16).reshape(16, 16, 128)
            tkst[:, p, high, :] = (k2 * hi).astype(BF16).reshape(16, 16, 128)
            v2 = dot(normed, wtq[:, 2 * D + p * 128 : 2 * D + (p + 1) * 128])
            tvst[:, p, frames, :] = (v2 * lo).astype(BF16).reshape(16, 16, 128)
            tvst[:, p, high, :] = (v2 * hi).astype(BF16).reshape(16, 16, 128)
        return carry

    lax.fori_loop(0, 8, group_step, 0)

    def token_step(t, carry):
        for p in range(4):
            tmix[t, :, p * 128 : (p + 1) * 128] = pair_attention(
                tq[t, :, p * 128 : (p + 1) * 128], tkst[t, p], tvst[t, p], ones_t[...], 128
            )
        tmix[t] = (xt[t].astype(F32) + dot(tmix[t], wto[...])).astype(BF16)
        return carry

    lax.fori_loop(0, 16, token_step, 0)

    def back_step(g, carry):
        frames = pl.ds(pl.multiple_of(g * 16, 16), 16)
        fg = tmix[:, frames, :].reshape(256, D)
        sbuf2[frames] = dot(perm[0], fg).astype(BF16).reshape(16, 16, D)
        slabs = dot(perm[1], fg).astype(BF16)
        rows = pl.ds(pl.multiple_of(g * 32, 32), 32)
        for s in range(8):
            cbuf[rows, s * D : (s + 1) * D] = slabs[s * 32 : (s + 1) * 32, :]
        return carry

    lax.fori_loop(0, 8, back_step, 0)

    mine = pl.ds(pl.multiple_of(me * 16, 16), 16)
    recv2[:, mine, :] = sbuf2[pl.ds(me * 4, 4)]
    for o in OFFSETS:
        to = peer(o)
        pltpu.make_async_remote_copy(
            src_ref=sbuf2.at[pl.ds(to * 4, 4)],
            dst_ref=recv2.at[:, mine, :],
            send_sem=ss2,
            recv_sem=rs2,
            device_id=(clip, to),
            device_id_type=MESH,
        ).start()

    for i in range(5, 9):
        wcopy[i].wait()
    c0[...] = dot(perm[2], dot(cbuf[...], wm[...]).astype(BF16)).astype(BF16)
    normed = (rms(c0[...].astype(F32)) * cgain[...]).astype(BF16)
    cq[...] = (dot(normed, wcq[:, 0:DC]) * QSCALE).astype(BF16)
    ck[...] = dot(normed, wcq[:, DC : 2 * DC]).astype(BF16)
    cv[...] = dot(normed, wcq[:, 2 * DC : 3 * DC]).astype(BF16)
    lane4 = lax.broadcasted_iota(jnp.int32, (64, 256), 1) >> 6
    block4 = jnp.concatenate(
        [jnp.where(lane4 == h, 1.0, 0.0).astype(BF16) for h in range(4)], axis=0
    )
    low = lax.broadcasted_iota(jnp.int32, (64, 128), 1) < HEAD

    def cell_step(b, carry):
        rows = pl.ds(pl.multiple_of(b * 64, 64), 64)
        for hg in range(4):
            lanes = slice(hg * 256, (hg + 1) * 256)
            k4, v4 = ck[rows, lanes], cv[rows, lanes]
            s = dot_t(cq[rows, lanes], jnp.concatenate([k4] * 4, axis=0) * block4)
            parts = []
            for half in range(2):
                sh = s[:, half * 128 : (half + 1) * 128]
                m_lo = jnp.max(jnp.where(low, sh, -jnp.inf), axis=-1, keepdims=True)
                m_hi = jnp.max(jnp.where(low, -jnp.inf, sh), axis=-1, keepdims=True)
                parts.append(jnp.exp2(sh - jnp.where(low, m_lo, m_hi)).astype(BF16))
            p = jnp.concatenate(parts, axis=1)
            o = dot(p, jnp.concatenate([v4] * 4, axis=0) * block4)
            cmix[rows, lanes] = (o / dot(p, block4)).astype(BF16)
        return carry

    lax.fori_loop(0, 4, cell_step, 0)
    coarse1 = (c0[...].astype(F32) + dot(cmix[...], wco[...])).astype(BF16)
    upped = dot(coarse1, wup[...]).astype(BF16)

    def pick(half):
        r = lax.broadcasted_iota(jnp.int32, (512, 256), 0)
        c = lax.broadcasted_iota(jnp.int32, (512, 256), 1)
        hit = (c == (r & 3) * 64 + (r >> 4) * 2 + ((r >> 2) & 1)) & (((r >> 3) & 1) == half)
        return jnp.where(hit, 1.0, 0.0).astype(BF16)

    zs[...] = (dot(pick(0), upped[:, :256]) + dot(pick(1), upped[:, 256:])).astype(BF16)
    zr[mine, :] = zs[mine, :]
    for o in OFFSETS:
        to = peer(o)
        pltpu.make_async_remote_copy(
            src_ref=zs.at[pl.ds(pl.multiple_of(to * 16, 16), 16), :],
            dst_ref=zr.at[mine, :],
            send_sem=ss3,
            recv_sem=rs3,
            device_id=(clip, to),
            device_id_type=MESH,
        ).start()

    pltpu.make_async_copy(
        recv2.at[:, pl.ds(0, 496), :], recv2.at[:, pl.ds(0, 496), :], rs2
    ).wait()
    pltpu.make_async_copy(zr.at[pl.ds(0, 496)], zr.at[pl.ds(0, 496)], rs3).wait()
    ocopy = []
    for j in range(2):
        for half in range(2):
            spread = onehot(256, 256, lambda r: (r & 240) + half * 8 + j * 4 + ((r >> 2) & 3))
            for k in range(2):
                rows = slice(k * 256, (k + 1) * 256)
                lanes = slice(half * 256, (half + 1) * 256)
                u = dot(spread, zr[rows, :])
                for f in (2 * j, 2 * j + 1):
                    vid[f, rows, lanes] = (recv2[f, rows, lanes].astype(F32) + u).astype(BF16)
        for f in (2 * j, 2 * j + 1):
            cp = pltpu.make_async_copy(vid.at[f], out.at[f], osem.at[f])
            cp.start()
            ocopy.append(cp)
    pltpu.make_async_copy(sbuf1.at[:, pl.ds(0, 496), :], sbuf1.at[:, pl.ds(0, 496), :], ss1).wait()
    pltpu.make_async_copy(sbuf2.at[pl.ds(0, 124)], sbuf2.at[pl.ds(0, 124)], ss2).wait()
    pltpu.make_async_copy(zs.at[pl.ds(0, 496)], zs.at[pl.ds(0, 496)], ss3).wait()
    for cp in ocopy:
        cp.wait()


def body(
    video, timestep, cond_weight, spatial_gain, spatial_qkv, spatial_out, temporal_gain,
    temporal_qkv, temporal_out, merge_weight, coarse_gain, coarse_qkv, coarse_out, up_weight,
):
    counter = jnp.arange(FREQ, dtype=F32)
    frequency = jnp.exp(counter * (-math.log(10000.0) / FREQ))
    angles = timestep.astype(F32)[0] * frequency
    emb = jnp.concatenate([jnp.sin(angles), jnp.cos(angles)])[:, None]
    any_, vm = pl.BlockSpec(memory_space=pl.ANY), pl.BlockSpec(memory_space=pltpu.VMEM)
    b = lambda *shape: pltpu.VMEM(shape, BF16)
    return pl.pallas_call(
        kernel,
        name="denoise",
        out_shape=jax.ShapeDtypeStruct(video.shape, BF16),
        in_specs=[any_, vm, any_, vm, any_, any_, vm, any_, any_, any_, vm, any_, any_, any_],
        out_specs=any_,
        scratch_shapes=[
            b(4, 512, D), b(128, 2048), b(D, 3 * D), b(D, D), b(D, 3 * D), b(D, D),
            b(8 * D, DC), b(DC, 3 * DC), b(DC, DC), b(DC, D),
            b(512, D), b(4, 1024, 128), b(4, 1024, 128), b(1024, 128), b(512, D),
            b(4, 512, D), b(128, 16, D),
            b(3, 256, 256), b(16, 128, D), b(16, 128, D), b(16, 4, 256, 128),
            b(16, 4, 256, 128), b(256, 128), b(16, 128, D),
            b(128, 16, D), b(256, 8 * D), b(4, 512, D),
            b(256, DC), b(256, DC), b(256, DC), b(256, DC), b(256, DC), b(512, 256), b(512, 256),
            pltpu.VMEM((1, 4 * D), F32),
            pltpu.SemaphoreType.DMA((9,)), pltpu.SemaphoreType.DMA((4,)),
            pltpu.SemaphoreType.DMA((4,)),
        ] + [pltpu.SemaphoreType.DMA] * 6,
        compiler_params=pltpu.CompilerParams(
            collective_id=0, has_side_effects=True, vmem_limit_bytes=67_000_000
        ),
    )(
        video, emb, cond_weight, spatial_gain[None], spatial_qkv, spatial_out,
        temporal_gain[None], temporal_qkv, temporal_out, merge_weight, coarse_gain[None],
        coarse_qkv, coarse_out, up_weight,
    )


def solution(mesh):
    return jax.shard_map(
        body,
        mesh=mesh,
        in_specs=(P(("clip", "frame"), None, None), P("clip")) + (P(),) * 12,
        out_specs=P(("clip", "frame"), None, None),
        check_vma=False,
    )
```

```python
import math

import jax
import jax.numpy as jnp
from jax import lax
from jax.experimental import pallas as pl
from jax.experimental.pallas import tpu as pltpu
from jax.sharding import PartitionSpec as P

D = 512
DC = 1024
HEAD = 64
FREQ = 64
GROUP = 32
MESH = pl.DeviceIdType.MESH
F32 = jnp.float32
BF16 = jnp.bfloat16
QSCALE = math.log2(math.e) / math.sqrt(HEAD)

OFFSETS = sorted(
    [(a, b, d) for a in range(4) for b in range(4) for d in range(2) if (a, b, d) != (0, 0, 0)],
    key=lambda o: -(min(o[0], 4 - o[0]) + min(o[1], 4 - o[1]) + o[2]),
)


def dot(a, b):
    return jnp.dot(a, b, preferred_element_type=F32)


def dot_t(a, b):
    return lax.dot_general(a, b, (((1,), (1,)), ((), ())), preferred_element_type=F32)


def onehot(rows, columns, column_of):
    r = lax.broadcasted_iota(jnp.int32, (rows, columns), 0)
    c = lax.broadcasted_iota(jnp.int32, (rows, columns), 1)
    return jnp.where(c == column_of(r), 1.0, 0.0).astype(BF16)


def rms(x):
    return x * lax.rsqrt(jnp.mean(x * x, axis=-1, keepdims=True) + 1e-06)


def finish_pair(s, vst, ones, keys):
    s_lo, s_hi = s[:, :keys], s[:, keys:]
    p_lo = jnp.exp2(s_lo - jnp.max(s_lo, axis=-1, keepdims=True)).astype(BF16)
    p_hi = jnp.exp2(s_hi - jnp.max(s_hi, axis=-1, keepdims=True)).astype(BF16)
    p = jnp.concatenate([p_lo, p_hi], axis=1)
    o = dot(p, jnp.concatenate([vst, ones], axis=1))
    return (o[:, :128] / o[:, 128:]).astype(BF16)


def pipelined(blocks, scores, finish):
    ahead = scores(*blocks[0])
    for n, block in enumerate(blocks):
        now = ahead
        if n + 1 < len(blocks):
            ahead = scores(*blocks[n + 1])
        finish(now, *block)


def kernel(
    video, emb, cond, sgain, sqkv, sout, tgain, tqkv, tout, merge, cgain, cqkv, cout, up,
    out,
    vid, wcond, wsq, wso, wtq, wto, wm, wcq, wco, wup,
    sq, skst, svst, ones_s, smix,
    sbuf1, recv1,
    perm, spread, xt, tq, tkst, tvst, ones_t, tmix,
    sbuf2, cbuf, recv2,
    c0, cq, ck, cv, cmix, zs, zr,
    modv, lsem, vsem, osem, ss1, rs1, ss2, rs2, ss3, rs3,
):
    clip = lax.axis_index("clip")
    me = lax.axis_index("frame")
    z, x, y = me // 8, lax.rem(me // 2, 4), lax.rem(me, 2)

    def peer(o):
        return lax.rem(z + o[0], 4) * 8 + lax.rem(x + o[1], 4) * 2 + lax.rem(y + o[2], 2)

    barrier = pltpu.get_barrier_semaphore()
    for o in OFFSETS:
        pl.semaphore_signal(barrier, inc=1, device_id=(clip, peer(o)), device_id_type=MESH)

    weights = [
        (cond, wcond), (sqkv, wsq), (sout, wso), (tqkv, wtq), (tout, wto),
        (merge, wm), (cqkv, wcq), (cout, wco), (up, wup),
    ]
    wcopy = [pltpu.make_async_copy(a, b, lsem.at[i]) for i, (a, b) in enumerate(weights)]
    vcopy = [pltpu.make_async_copy(video.at[f], vid.at[f], vsem.at[f]) for f in range(4)]
    vcopy[0].start()
    for i in range(3):
        wcopy[i].start()
    for f in range(1, 4):
        vcopy[f].start()

    lane = lax.broadcasted_iota(jnp.int32, (1, 128), 1)
    lo = jnp.where(lane < HEAD, 1.0, 0.0).astype(F32)
    hi = 1.0 - lo
    ones_s[0:512, :] = jnp.broadcast_to(lo, (512, 128)).astype(BF16)
    ones_s[512:1024, :] = jnp.broadcast_to(hi, (512, 128)).astype(BF16)
    ones_t[0:128, :] = jnp.broadcast_to(lo, (128, 128)).astype(BF16)
    ones_t[128:256, :] = jnp.broadcast_to(hi, (128, 128)).astype(BF16)
    perm[0] = onehot(256, 256, lambda r: (r & 15) * 16 + (r >> 4))
    perm[1] = onehot(
        256, 256, lambda r: ((r >> 2) & 3) * 64 + ((r >> 4) & 3) * 16 + (r >> 6) * 4 + (r & 3)
    )
    for half in range(2):
        spread[half] = onehot(
            256, 64,
            lambda r: ((r >> 4) & 3) * 16 + half * 8 + (r >> 7) * 4 + ((r >> 2) & 3),
        )

    wcopy[0].wait()
    e1 = emb[...].astype(BF16).astype(F32)
    e2 = (emb[...] - e1).astype(BF16).astype(F32)
    e3 = emb[...] - e1 - e2
    piece = lax.broadcasted_iota(jnp.int32, (8, 128), 0)
    pieces = jnp.where(piece == 0, e1, jnp.where(piece == 1, e2, jnp.where(piece == 2, e3, 0.0)))
    modv[...] = jnp.sum(dot(pieces.astype(BF16), wcond[...]), axis=0, keepdims=True)
    sg = sgain[...] * (1.0 + modv[:, 0:D])
    shs = modv[:, D : 2 * D]
    tg = tgain[...] * (1.0 + modv[:, 2 * D : 3 * D])
    sht = modv[:, 3 * D : 4 * D]

    wcopy[1].wait()
    for i in range(3, 9):
        wcopy[i].start()
    pl.semaphore_wait(barrier, len(OFFSETS))

    def frame_step(f, carry):
        pltpu.make_async_copy(video.at[f], vid.at[f], vsem.at[f]).wait()
        xf = vid[f].astype(F32)
        normed = (rms(xf) * sg + shs).astype(BF16)
        sq[...] = (dot(normed, wsq[:, 0:D]) * QSCALE).astype(BF16)
        for p in range(4):
            k2 = dot(normed, wsq[:, D + p * 128 : D + (p + 1) * 128])
            skst[p, 0:512] = (k2 * lo).astype(BF16)
            skst[p, 512:1024] = (k2 * hi).astype(BF16)
            v2 = dot(normed, wsq[:, 2 * D + p * 128 : 2 * D + (p + 1) * 128])
            svst[p, 0:512] = (v2 * lo).astype(BF16)
            svst[p, 512:1024] = (v2 * hi).astype(BF16)

        def scores(p, i):
            return dot_t(sq[i * 256 : (i + 1) * 256, p * 128 : (p + 1) * 128], skst[p])

        def finish(v, p, i):
            smix[i * 256 : (i + 1) * 256, p * 128 : (p + 1) * 128] = finish_pair(
                v, svst[p], ones_s[...], 512
            )

        pipelined([(p, i) for p in range(4) for i in range(2)], scores, finish)

        @pl.when(f == 0)
        def _():
            wcopy[2].wait()

        sbuf1[f] = (vid[f].astype(F32) + dot(smix[...], wso[...])).astype(BF16)
        own = pl.ds(pl.multiple_of(me * 16, 16), 16)
        recv1[f * GROUP + me] = sbuf1[f, own, :]
        for o in OFFSETS:
            to = peer(o)
            pltpu.make_async_remote_copy(
                src_ref=sbuf1.at[f, pl.ds(pl.multiple_of(to * 16, 16), 16), :],
                dst_ref=recv1.at[f * GROUP + me],
                send_sem=ss1,
                recv_sem=rs1.at[f],
                device_id=(clip, to),
                device_id_type=MESH,
            ).start()
        return carry

    lax.fori_loop(0, 4, frame_step, 0)

    wcopy[3].wait()
    wcopy[4].wait()

    def group_step(j, carry):
        pltpu.make_async_copy(recv1.at[pl.ds(0, 31)], recv1.at[pl.ds(0, 31)], rs1.at[j]).wait()
        for sb in range(2):
            base = j * GROUP + sb * 16
            frames = pl.ds(pl.multiple_of(base, 16), 16)
            high = pl.ds(pl.multiple_of(128 + base, 16), 16)
            yg = dot(perm[0], recv1[frames].reshape(256, D))
            xt[:, frames, :] = yg.astype(BF16).reshape(16, 16, D)
            normed = (rms(yg) * tg + sht).astype(BF16)
            tq[:, frames, :] = (dot(normed, wtq[:, 0:D]) * QSCALE).astype(BF16).reshape(16, 16, D)
            for p in range(4):
                k2 = dot(normed, wtq[:, D + p * 128 : D + (p + 1) * 128])
                tkst[:, p, frames, :] = (k2 * lo).astype(BF16).reshape(16, 16, 128)
                tkst[:, p, high, :] = (k2 * hi).astype(BF16).reshape(16, 16, 128)
                v2 = dot(normed, wtq[:, 2 * D + p * 128 : 2 * D + (p + 1) * 128])
                tvst[:, p, frames, :] = (v2 * lo).astype(BF16).reshape(16, 16, 128)
                tvst[:, p, high, :] = (v2 * hi).astype(BF16).reshape(16, 16, 128)
        return carry

    lax.fori_loop(0, 4, group_step, 0)

    def token_step(c, carry):
        def scores(q, p):
            return dot_t(tq[c * 4 + q, :, p * 128 : (p + 1) * 128], tkst[c * 4 + q, p])

        def finish(v, q, p):
            tmix[q, :, p * 128 : (p + 1) * 128] = finish_pair(
                v, tvst[c * 4 + q, p], ones_t[...], 128
            )

        pipelined([(q, p) for q in range(4) for p in range(4)], scores, finish)
        for q in range(4):
            tmix[q] = (xt[c * 4 + q].astype(F32) + dot(tmix[q], wto[...])).astype(BF16)
        for sb in range(2):
            fg = jnp.concatenate(
                [
                    tmix[q, j * GROUP + sb * 16 : j * GROUP + (sb + 1) * 16, :]
                    for j in range(4) for q in range(4)
                ],
                axis=0,
            )
            sbuf2[c, sb * 16 : (sb + 1) * 16] = dot(perm[0], fg).astype(BF16).reshape(16, 16, D)
        recv2[c, me] = sbuf2[c, me]
        for o in OFFSETS:
            to = peer(o)
            pltpu.make_async_remote_copy(
                src_ref=sbuf2.at[c, to],
                dst_ref=recv2.at[c, me],
                send_sem=ss2,
                recv_sem=rs2,
                device_id=(clip, to),
                device_id_type=MESH,
            ).start()
        for d in range(2):
            for q in range(4):
                for jh in range(2):
                    j = 2 * jh + d
                    cbuf[
                        pl.ds(pl.multiple_of(c * 64 + jh * 32, 32), 32),
                        (d * 4 + q) * D : (d * 4 + q + 1) * D,
                    ] = tmix[q, j * GROUP : (j + 1) * GROUP, :]
        return carry

    lax.fori_loop(0, 4, token_step, 0)
    mine = pl.ds(pl.multiple_of(me * 16, 16), 16)

    for i in range(5, 9):
        wcopy[i].wait()
    c0[...] = dot(cbuf[...], wm[...]).astype(BF16)
    normed = (rms(c0[...].astype(F32)) * cgain[...]).astype(BF16)
    cq[...] = (dot(normed, wcq[:, 0:DC]) * QSCALE).astype(BF16)
    ck[...] = dot(normed, wcq[:, DC : 2 * DC]).astype(BF16)
    cv[...] = dot(normed, wcq[:, 2 * DC : 3 * DC]).astype(BF16)
    lane4 = lax.broadcasted_iota(jnp.int32, (64, 256), 1) >> 6
    block4 = jnp.concatenate(
        [jnp.where(lane4 == h, 1.0, 0.0).astype(BF16) for h in range(4)], axis=0
    )
    low = lax.broadcasted_iota(jnp.int32, (64, 128), 1) < HEAD

    def cell_scores(b, hg):
        rows, lanes = slice(b * 64, (b + 1) * 64), slice(hg * 256, (hg + 1) * 256)
        return dot_t(cq[rows, lanes], jnp.concatenate([ck[rows, lanes]] * 4, axis=0) * block4)

    def cell_finish(s, b, hg):
        rows, lanes = slice(b * 64, (b + 1) * 64), slice(hg * 256, (hg + 1) * 256)
        parts = []
        for half in range(2):
            sh = s[:, half * 128 : (half + 1) * 128]
            m_lo = jnp.max(jnp.where(low, sh, -jnp.inf), axis=-1, keepdims=True)
            m_hi = jnp.max(jnp.where(low, -jnp.inf, sh), axis=-1, keepdims=True)
            parts.append(jnp.exp2(sh - jnp.where(low, m_lo, m_hi)).astype(BF16))
        p = jnp.concatenate(parts, axis=1)
        o = dot(p, jnp.concatenate([cv[rows, lanes]] * 4, axis=0) * block4)
        cmix[rows, lanes] = (o / dot(p, block4)).astype(BF16)

    pipelined([(b, hg) for b in range(4) for hg in range(4)], cell_scores, cell_finish)
    coarse1 = (c0[...].astype(F32) + dot(cmix[...], wco[...])).astype(BF16)
    upped = dot(coarse1, wup[...]).astype(BF16)

    def pick(half):
        r = lax.broadcasted_iota(jnp.int32, (512, 256), 0)
        c = lax.broadcasted_iota(jnp.int32, (512, 256), 1)
        hit = (c == (r & 3) * 64 + ((r >> 2) & 1) * 32 + (r >> 4)) & (((r >> 3) & 1) == half)
        return jnp.where(hit, 1.0, 0.0).astype(BF16)

    zs[...] = (dot(pick(0), upped[:, :256]) + dot(pick(1), upped[:, 256:])).astype(BF16)
    zr[mine, :] = zs[mine, :]
    for o in OFFSETS:
        to = peer(o)
        pltpu.make_async_remote_copy(
            src_ref=zs.at[pl.ds(pl.multiple_of(to * 16, 16), 16), :],
            dst_ref=zr.at[mine, :],
            send_sem=ss3,
            recv_sem=rs3,
            device_id=(clip, to),
            device_id_type=MESH,
        ).start()

    pltpu.make_async_copy(recv2.at[:, pl.ds(0, 31)], recv2.at[:, pl.ds(0, 31)], rs2).wait()
    pltpu.make_async_copy(zr.at[pl.ds(0, 496)], zr.at[pl.ds(0, 496)], rs3).wait()
    ocopy = []
    for sb in range(8):
        got = jnp.concatenate(
            [recv2[c, sb * 4 : (sb + 1) * 4].reshape(64, D) for c in range(4)], axis=0
        )
        coarse = zr[sb * 64 : (sb + 1) * 64, :]
        for half in range(2):
            lanes = slice(half * 256, (half + 1) * 256)
            total = dot(perm[1], got[:, lanes]) + dot(spread[half], coarse)
            for j in range(4):
                vid[j, sb * 64 : (sb + 1) * 64, lanes] = total[j * 64 : (j + 1) * 64].astype(BF16)
        rows = pl.ds(sb * 64, 64)
        cp = pltpu.make_async_copy(vid.at[:, rows, :], out.at[:, rows, :], osem.at[sb])
        cp.start()
        ocopy.append(cp)
    pltpu.make_async_copy(sbuf1.at[:, pl.ds(0, 496), :], sbuf1.at[:, pl.ds(0, 496), :], ss1).wait()
    pltpu.make_async_copy(sbuf2.at[:, pl.ds(0, 31)], sbuf2.at[:, pl.ds(0, 31)], ss2).wait()
    pltpu.make_async_copy(zs.at[pl.ds(0, 496)], zs.at[pl.ds(0, 496)], ss3).wait()
    for cp in ocopy:
        cp.wait()


def body(
    video, timestep, cond_weight, spatial_gain, spatial_qkv, spatial_out, temporal_gain,
    temporal_qkv, temporal_out, merge_weight, coarse_gain, coarse_qkv, coarse_out, up_weight,
):
    counter = jnp.arange(FREQ, dtype=F32)
    frequency = jnp.exp(counter * (-math.log(10000.0) / FREQ))
    angles = timestep.astype(F32)[0] * frequency
    emb = jnp.concatenate([jnp.sin(angles), jnp.cos(angles)])[None]
    any_, vm = pl.BlockSpec(memory_space=pl.ANY), pl.BlockSpec(memory_space=pltpu.VMEM)
    b = lambda *shape: pltpu.VMEM(shape, BF16)
    return pl.pallas_call(
        kernel,
        name="denoise",
        out_shape=jax.ShapeDtypeStruct(video.shape, BF16),
        in_specs=[any_, vm, any_, vm, any_, any_, vm, any_, any_, any_, vm, any_, any_, any_],
        out_specs=any_,
        scratch_shapes=[
            b(4, 512, D), b(128, 2048), b(D, 3 * D), b(D, D), b(D, 3 * D), b(D, D),
            b(8 * D, DC), b(DC, 3 * DC), b(DC, DC), b(DC, D),
            b(512, D), b(4, 1024, 128), b(4, 1024, 128), b(1024, 128), b(512, D),
            b(4, 512, D), b(128, 16, D),
            b(2, 256, 256), b(2, 256, 64), b(16, 128, D), b(16, 128, D), b(16, 4, 256, 128),
            b(16, 4, 256, 128), b(256, 128), b(4, 128, D),
            b(4, 32, 16, D), b(256, 8 * D), b(4, 32, 16, D),
            b(256, DC), b(256, DC), b(256, DC), b(256, DC), b(256, DC), b(512, 256), b(512, 256),
            pltpu.VMEM((1, 4 * D), F32),
            pltpu.SemaphoreType.DMA((9,)), pltpu.SemaphoreType.DMA((4,)),
            pltpu.SemaphoreType.DMA((8,)),
            pltpu.SemaphoreType.DMA, pltpu.SemaphoreType.DMA((4,)),
        ] + [pltpu.SemaphoreType.DMA] * 4,
        compiler_params=pltpu.CompilerParams(
            collective_id=0, has_side_effects=True, vmem_limit_bytes=67_000_000
        ),
    )(
        video, emb, cond_weight, spatial_gain[None], spatial_qkv, spatial_out,
        temporal_gain[None], temporal_qkv, temporal_out, merge_weight, coarse_gain[None],
        coarse_qkv, coarse_out, up_weight,
    )


def solution(mesh):
    return jax.shard_map(
        body,
        mesh=mesh,
        in_specs=(P(("clip", "frame"), None, None), P("clip")) + (P(),) * 12,
        out_specs=P(("clip", "frame"), None, None),
        check_vma=False,
    )
```

```python
import math

import jax
import jax.numpy as jnp
from jax import lax
from jax.experimental import pallas as pl
from jax.experimental.pallas import tpu as pltpu
from jax.sharding import PartitionSpec as P

D = 512
DC = 1024
HEAD = 64
FREQ = 64
GROUP = 32
MESH = pl.DeviceIdType.MESH
F32 = jnp.float32
BF16 = jnp.bfloat16
QSCALE = math.log2(math.e) / math.sqrt(HEAD)

OFFSETS = sorted(
    [(a, b, d) for a in range(4) for b in range(4) for d in range(2) if (a, b, d) != (0, 0, 0)],
    key=lambda o: -(min(o[0], 4 - o[0]) + min(o[1], 4 - o[1]) + o[2]),
)


def dot(a, b):
    return jnp.dot(a, b, preferred_element_type=F32)


def dot_t(a, b):
    return lax.dot_general(a, b, (((1,), (1,)), ((), ())), preferred_element_type=F32)


def onehot(rows, columns, column_of):
    r = lax.broadcasted_iota(jnp.int32, (rows, columns), 0)
    c = lax.broadcasted_iota(jnp.int32, (rows, columns), 1)
    return jnp.where(c == column_of(r), 1.0, 0.0).astype(BF16)


def rms(x):
    return x * lax.rsqrt(jnp.mean(x * x, axis=-1, keepdims=True) + 1e-06)


def finish_pair(s, vst, ones, keys):
    s_lo, s_hi = s[:, :keys], s[:, keys:]
    p_lo = jnp.exp2(s_lo - jnp.max(s_lo, axis=-1, keepdims=True)).astype(BF16)
    p_hi = jnp.exp2(s_hi - jnp.max(s_hi, axis=-1, keepdims=True)).astype(BF16)
    p = jnp.concatenate([p_lo, p_hi], axis=1)
    o = dot(p, jnp.concatenate([vst, ones], axis=1))
    return (o[:, :128] / o[:, 128:]).astype(BF16)


def pipelined(blocks, scores, finish):
    ahead = scores(*blocks[0])
    for n, block in enumerate(blocks):
        now = ahead
        if n + 1 < len(blocks):
            ahead = scores(*blocks[n + 1])
        finish(now, *block)


def kernel(
    video, emb, cond, sgain, sqkv, sout, tgain, tqkv, tout, merge, cgain, cqkv, cout, up,
    recv2, zr,
    vid, wcond, wsq, wso, wtq, wto, wm, wcq, wco, wup,
    sq, skst, svst, ones_s, smix,
    sbuf1, recv1,
    perm, xt, tq, tkst, tvst, ones_t, tmix,
    sbuf2, cbuf,
    c0, cq, ck, cv, cmix, zs,
    modv, lsem, vsem, osem, ss1, rs1, ss2, rs2, ss3, rs3,
):
    clip = lax.axis_index("clip")
    me = lax.axis_index("frame")
    z, x, y = me // 8, lax.rem(me // 2, 4), lax.rem(me, 2)

    def peer(o):
        return lax.rem(z + o[0], 4) * 8 + lax.rem(x + o[1], 4) * 2 + lax.rem(y + o[2], 2)

    barrier = pltpu.get_barrier_semaphore()
    for o in OFFSETS:
        pl.semaphore_signal(barrier, inc=1, device_id=(clip, peer(o)), device_id_type=MESH)

    weights = [
        (cond, wcond), (sqkv, wsq), (sout, wso), (tqkv, wtq), (tout, wto),
        (merge, wm), (cqkv, wcq), (cout, wco), (up, wup),
    ]
    wcopy = [pltpu.make_async_copy(a, b, lsem.at[i]) for i, (a, b) in enumerate(weights)]
    vcopy = [pltpu.make_async_copy(video.at[f], vid.at[f], vsem.at[f]) for f in range(4)]
    vcopy[0].start()
    for i in range(3):
        wcopy[i].start()
    for f in range(1, 4):
        vcopy[f].start()

    lane = lax.broadcasted_iota(jnp.int32, (1, 128), 1)
    lo = jnp.where(lane < HEAD, 1.0, 0.0).astype(F32)
    hi = 1.0 - lo
    ones_s[0:512, :] = jnp.broadcast_to(lo, (512, 128)).astype(BF16)
    ones_s[512:1024, :] = jnp.broadcast_to(hi, (512, 128)).astype(BF16)
    ones_t[0:128, :] = jnp.broadcast_to(lo, (128, 128)).astype(BF16)
    ones_t[128:256, :] = jnp.broadcast_to(hi, (128, 128)).astype(BF16)
    perm[...] = onehot(256, 256, lambda r: (r & 15) * 16 + (r >> 4))

    wcopy[0].wait()
    e1 = emb[...].astype(BF16).astype(F32)
    e2 = (emb[...] - e1).astype(BF16).astype(F32)
    e3 = emb[...] - e1 - e2
    piece = lax.broadcasted_iota(jnp.int32, (8, 128), 0)
    pieces = jnp.where(piece == 0, e1, jnp.where(piece == 1, e2, jnp.where(piece == 2, e3, 0.0)))
    modv[...] = jnp.sum(dot(pieces.astype(BF16), wcond[...]), axis=0, keepdims=True)
    sg = sgain[...] * (1.0 + modv[:, 0:D])
    shs = modv[:, D : 2 * D]
    tg = tgain[...] * (1.0 + modv[:, 2 * D : 3 * D])
    sht = modv[:, 3 * D : 4 * D]

    wcopy[1].wait()
    wcopy[2].wait()
    for i in range(3, 9):
        wcopy[i].start()

    def frame_step(f, carry):
        pltpu.make_async_copy(video.at[f], vid.at[f], vsem.at[f]).wait()
        xf = vid[f].astype(F32)
        normed = (rms(xf) * sg + shs).astype(BF16)
        sq[...] = (dot(normed, wsq[:, 0:D]) * QSCALE).astype(BF16)
        for p in range(4):
            k2 = dot(normed, wsq[:, D + p * 128 : D + (p + 1) * 128])
            skst[p, 0:512] = (k2 * lo).astype(BF16)
            skst[p, 512:1024] = (k2 * hi).astype(BF16)
            v2 = dot(normed, wsq[:, 2 * D + p * 128 : 2 * D + (p + 1) * 128])
            svst[p, 0:512] = (v2 * lo).astype(BF16)
            svst[p, 512:1024] = (v2 * hi).astype(BF16)

        @pl.when(f == 0)
        def _():
            pl.semaphore_wait(barrier, len(OFFSETS))

        def rows_of(dz):
            return pl.ds(pl.multiple_of(lax.rem(z + dz, 4) * 128, 128), 128)

        def scores(dz, p):
            return dot_t(sq[rows_of(dz), p * 128 : (p + 1) * 128], skst[p])

        def finish(v, dz, p):
            rows = rows_of(dz)
            smix[rows, p * 128 : (p + 1) * 128] = finish_pair(v, svst[p], ones_s[...], 512)
            if p < 3:
                return
            sbuf1[f, rows, :] = (vid[f, rows, :].astype(F32) + dot(smix[rows, :], wso[...])).astype(BF16)
            if dz == 0:
                own = pl.ds(pl.multiple_of(me * 16, 16), 16)
                recv1[f * GROUP + me] = sbuf1[f, own, :]
            for o in OFFSETS:
                if o[0] == dz:
                    to = peer(o)
                    pltpu.make_async_remote_copy(
                        src_ref=sbuf1.at[f, pl.ds(pl.multiple_of(to * 16, 16), 16), :],
                        dst_ref=recv1.at[f * GROUP + me],
                        send_sem=ss1,
                        recv_sem=rs1.at[f],
                        device_id=(clip, to),
                        device_id_type=MESH,
                    ).start()

        pipelined([(dz, p) for dz in (2, 1, 3, 0) for p in range(4)], scores, finish)
        return carry

    lax.fori_loop(0, 4, frame_step, 0)

    wcopy[3].wait()
    wcopy[4].wait()

    def group_step(j, carry):
        pltpu.make_async_copy(recv1.at[pl.ds(0, 31)], recv1.at[pl.ds(0, 31)], rs1.at[j]).wait()
        for sb in range(2):
            base = j * GROUP + sb * 16
            frames = pl.ds(pl.multiple_of(base, 16), 16)
            high = pl.ds(pl.multiple_of(128 + base, 16), 16)
            yg = dot(perm[...], recv1[frames].reshape(256, D))
            xt[:, frames, :] = yg.astype(BF16).reshape(16, 16, D)
            normed = (rms(yg) * tg + sht).astype(BF16)
            tq[:, frames, :] = (dot(normed, wtq[:, 0:D]) * QSCALE).astype(BF16).reshape(16, 16, D)
            for p in range(4):
                k2 = dot(normed, wtq[:, D + p * 128 : D + (p + 1) * 128])
                tkst[:, p, frames, :] = (k2 * lo).astype(BF16).reshape(16, 16, 128)
                tkst[:, p, high, :] = (k2 * hi).astype(BF16).reshape(16, 16, 128)
                v2 = dot(normed, wtq[:, 2 * D + p * 128 : 2 * D + (p + 1) * 128])
                tvst[:, p, frames, :] = (v2 * lo).astype(BF16).reshape(16, 16, 128)
                tvst[:, p, high, :] = (v2 * hi).astype(BF16).reshape(16, 16, 128)
        return carry

    lax.fori_loop(0, 4, group_step, 0)

    def token_step(c, carry):
        def scores(q, p):
            return dot_t(tq[c * 4 + q, :, p * 128 : (p + 1) * 128], tkst[c * 4 + q, p])

        def finish(v, q, p):
            tmix[q, :, p * 128 : (p + 1) * 128] = finish_pair(
                v, tvst[c * 4 + q, p], ones_t[...], 128
            )

        pipelined([(q, p) for q in range(4) for p in range(4)], scores, finish)
        for q in range(4):
            tmix[q] = (xt[c * 4 + q].astype(F32) + dot(tmix[q], wto[...])).astype(BF16)
        for sb in range(2):
            fg = jnp.concatenate(
                [
                    tmix[q, j * GROUP + sb * 16 : j * GROUP + (sb + 1) * 16, :]
                    for j in range(4) for q in range(4)
                ],
                axis=0,
            )
            sbuf2[c, sb * 16 : (sb + 1) * 16] = dot(perm[...], fg).astype(BF16).reshape(16, 16, D)
        pltpu.make_async_copy(sbuf2.at[c, me], recv2.at[c, me], osem.at[c]).start()
        for o in OFFSETS:
            to = peer(o)
            pltpu.make_async_remote_copy(
                src_ref=sbuf2.at[c, to],
                dst_ref=recv2.at[c, me],
                send_sem=ss2,
                recv_sem=rs2,
                device_id=(clip, to),
                device_id_type=MESH,
            ).start()
        for d in range(2):
            for q in range(4):
                for jh in range(2):
                    j = 2 * jh + d
                    cbuf[
                        pl.ds(pl.multiple_of(c * 64 + jh * 32, 32), 32),
                        (d * 4 + q) * D : (d * 4 + q + 1) * D,
                    ] = tmix[q, j * GROUP : (j + 1) * GROUP, :]
        return carry

    lax.fori_loop(0, 4, token_step, 0)
    mine = pl.ds(pl.multiple_of(me * 16, 16), 16)

    for i in range(5, 9):
        wcopy[i].wait()
    c0[...] = dot(cbuf[...], wm[...]).astype(BF16)
    normed = (rms(c0[...].astype(F32)) * cgain[...]).astype(BF16)
    cq[...] = (dot(normed, wcq[:, 0:DC]) * QSCALE).astype(BF16)
    ck[...] = dot(normed, wcq[:, DC : 2 * DC]).astype(BF16)
    cv[...] = dot(normed, wcq[:, 2 * DC : 3 * DC]).astype(BF16)
    lane4 = lax.broadcasted_iota(jnp.int32, (64, 256), 1) >> 6
    block4 = jnp.concatenate(
        [jnp.where(lane4 == h, 1.0, 0.0).astype(BF16) for h in range(4)], axis=0
    )
    low = lax.broadcasted_iota(jnp.int32, (64, 128), 1) < HEAD

    def cell_scores(b, hg):
        rows, lanes = slice(b * 64, (b + 1) * 64), slice(hg * 256, (hg + 1) * 256)
        return dot_t(cq[rows, lanes], jnp.concatenate([ck[rows, lanes]] * 4, axis=0) * block4)

    def cell_finish(s, b, hg):
        rows, lanes = slice(b * 64, (b + 1) * 64), slice(hg * 256, (hg + 1) * 256)
        parts = []
        for half in range(2):
            sh = s[:, half * 128 : (half + 1) * 128]
            m_lo = jnp.max(jnp.where(low, sh, -jnp.inf), axis=-1, keepdims=True)
            m_hi = jnp.max(jnp.where(low, -jnp.inf, sh), axis=-1, keepdims=True)
            parts.append(jnp.exp2(sh - jnp.where(low, m_lo, m_hi)).astype(BF16))
        p = jnp.concatenate(parts, axis=1)
        o = dot(p, jnp.concatenate([cv[rows, lanes]] * 4, axis=0) * block4)
        cmix[rows, lanes] = (o / dot(p, block4)).astype(BF16)

    pipelined([(b, hg) for b in range(4) for hg in range(4)], cell_scores, cell_finish)
    coarse1 = (c0[...].astype(F32) + dot(cmix[...], wco[...])).astype(BF16)
    upped = dot(coarse1, wup[...]).astype(BF16)

    def pick(half):
        r = lax.broadcasted_iota(jnp.int32, (512, 256), 0)
        c = lax.broadcasted_iota(jnp.int32, (512, 256), 1)
        hit = (c == (r & 3) * 64 + ((r >> 2) & 1) * 32 + (r >> 4)) & (((r >> 3) & 1) == half)
        return jnp.where(hit, 1.0, 0.0).astype(BF16)

    zs[...] = (dot(pick(0), upped[:, :256]) + dot(pick(1), upped[:, 256:])).astype(BF16)
    own_z = pltpu.make_async_copy(zs.at[mine], zr.at[mine], osem.at[4])
    own_z.start()
    for o in OFFSETS:
        to = peer(o)
        pltpu.make_async_remote_copy(
            src_ref=zs.at[pl.ds(pl.multiple_of(to * 16, 16), 16), :],
            dst_ref=zr.at[mine, :],
            send_sem=ss3,
            recv_sem=rs3,
            device_id=(clip, to),
            device_id_type=MESH,
        ).start()

    pltpu.make_async_copy(recv2.at[:, pl.ds(0, 31)], recv2.at[:, pl.ds(0, 31)], rs2).wait()
    pltpu.make_async_copy(zr.at[pl.ds(0, 496)], zr.at[pl.ds(0, 496)], rs3).wait()
    pltpu.make_async_copy(sbuf1.at[:, pl.ds(0, 496), :], sbuf1.at[:, pl.ds(0, 496), :], ss1).wait()
    pltpu.make_async_copy(sbuf2.at[:, pl.ds(0, 31)], sbuf2.at[:, pl.ds(0, 31)], ss2).wait()
    pltpu.make_async_copy(zs.at[pl.ds(0, 496)], zs.at[pl.ds(0, 496)], ss3).wait()
    for c in range(4):
        pltpu.make_async_copy(sbuf2.at[c, me], recv2.at[c, me], osem.at[c]).wait()
    own_z.wait()


def combine(fine, coarse, out, got, zin, res, perm, spread, isem, osem):
    def part(sb):
        return pl.ds(sb * 4, 4)

    zcopy = pltpu.make_async_copy(coarse, zin, isem.at[8])
    zcopy.start()
    icopy = [
        pltpu.make_async_copy(fine.at[:, part(sb)], got.at[:, part(sb)], isem.at[sb])
        for sb in range(8)
    ]
    for cp in icopy:
        cp.start()
    perm[...] = onehot(
        256, 256, lambda r: ((r >> 2) & 3) * 64 + ((r >> 4) & 3) * 16 + (r >> 6) * 4 + (r & 3)
    )
    for half in range(2):
        spread[half] = onehot(
            256, 64,
            lambda r: ((r >> 4) & 3) * 16 + half * 8 + (r >> 7) * 4 + ((r >> 2) & 3),
        )
    zcopy.wait()
    ocopy = []
    for sb in range(8):
        icopy[sb].wait()
        rows = slice(sb * 64, (sb + 1) * 64)
        cells = jnp.concatenate([got[c, part(sb)].reshape(64, D) for c in range(4)], axis=0)
        for half in range(2):
            lanes = slice(half * 256, (half + 1) * 256)
            total = dot(perm[...], cells[:, lanes]) + dot(spread[half], zin[rows, :])
            for j in range(4):
                res[j, rows, lanes] = total[j * 64 : (j + 1) * 64].astype(BF16)
        cp = pltpu.make_async_copy(
            res.at[:, pl.ds(sb * 64, 64), :], out.at[:, pl.ds(sb * 64, 64), :], osem.at[sb]
        )
        cp.start()
        ocopy.append(cp)
    for cp in ocopy:
        cp.wait()


def body(
    video, timestep, cond_weight, spatial_gain, spatial_qkv, spatial_out, temporal_gain,
    temporal_qkv, temporal_out, merge_weight, coarse_gain, coarse_qkv, coarse_out, up_weight,
):
    counter = jnp.arange(FREQ, dtype=F32)
    frequency = jnp.exp(counter * (-math.log(10000.0) / FREQ))
    angles = timestep.astype(F32)[0] * frequency
    emb = jnp.concatenate([jnp.sin(angles), jnp.cos(angles)])[None]
    any_, vm = pl.BlockSpec(memory_space=pl.ANY), pl.BlockSpec(memory_space=pltpu.VMEM)
    b = lambda *shape: pltpu.VMEM(shape, BF16)
    fine, coarse = pl.pallas_call(
        kernel,
        name="denoise",
        out_shape=[
            jax.ShapeDtypeStruct((4, GROUP, 16, D), BF16),
            jax.ShapeDtypeStruct((512, 256), BF16),
        ],
        in_specs=[any_, vm, any_, vm, any_, any_, vm, any_, any_, any_, vm, any_, any_, any_],
        out_specs=[any_, any_],
        scratch_shapes=[
            b(4, 512, D), b(128, 2048), b(D, 3 * D), b(D, D), b(D, 3 * D), b(D, D),
            b(8 * D, DC), b(DC, 3 * DC), b(DC, DC), b(DC, D),
            b(512, D), b(4, 1024, 128), b(4, 1024, 128), b(1024, 128), b(512, D),
            b(4, 512, D), b(128, 16, D),
            b(256, 256), b(16, 128, D), b(16, 128, D), b(16, 4, 256, 128),
            b(16, 4, 256, 128), b(256, 128), b(4, 128, D),
            b(4, 32, 16, D), b(256, 8 * D),
            b(256, DC), b(256, DC), b(256, DC), b(256, DC), b(256, DC), b(512, 256),
            pltpu.VMEM((1, 4 * D), F32),
            pltpu.SemaphoreType.DMA((9,)), pltpu.SemaphoreType.DMA((4,)),
            pltpu.SemaphoreType.DMA((8,)),
            pltpu.SemaphoreType.DMA, pltpu.SemaphoreType.DMA((4,)),
        ] + [pltpu.SemaphoreType.DMA] * 4,
        compiler_params=pltpu.CompilerParams(
            collective_id=0, has_side_effects=True, vmem_limit_bytes=67_000_000
        ),
    )(
        video, emb, cond_weight, spatial_gain[None], spatial_qkv, spatial_out,
        temporal_gain[None], temporal_qkv, temporal_out, merge_weight, coarse_gain[None],
        coarse_qkv, coarse_out, up_weight,
    )
    return pl.pallas_call(
        combine,
        name="combine",
        out_shape=jax.ShapeDtypeStruct(video.shape, BF16),
        in_specs=[any_, any_],
        out_specs=any_,
        scratch_shapes=[
            b(4, GROUP, 16, D), b(512, 256), b(4, 512, D), b(256, 256), b(2, 256, 64),
            pltpu.SemaphoreType.DMA((9,)), pltpu.SemaphoreType.DMA((8,)),
        ],
    )(fine, coarse)


def solution(mesh):
    return jax.shard_map(
        body,
        mesh=mesh,
        in_specs=(P(("clip", "frame"), None, None), P("clip")) + (P(),) * 12,
        out_specs=P(("clip", "frame"), None, None),
        check_vma=False,
    )
```

```python
import math

import jax
import jax.numpy as jnp
from jax import lax
from jax.experimental import pallas as pl
from jax.experimental.pallas import tpu as pltpu
from jax.sharding import PartitionSpec as P

D = 512
DC = 1024
HEAD = 64
FREQ = 64
GROUP = 32
MESH = pl.DeviceIdType.MESH
F32 = jnp.float32
BF16 = jnp.bfloat16
QSCALE = math.log2(math.e) / math.sqrt(HEAD)

OFFSETS = sorted(
    [(a, b, d) for a in range(4) for b in range(4) for d in range(2) if (a, b, d) != (0, 0, 0)],
    key=lambda o: -(min(o[0], 4 - o[0]) + min(o[1], 4 - o[1]) + o[2]),
)


def dot(a, b):
    return jnp.dot(a, b, preferred_element_type=F32)


def dot_t(a, b):
    return lax.dot_general(a, b, (((1,), (1,)), ((), ())), preferred_element_type=F32)


def onehot(rows, columns, column_of, keep=None):
    r = lax.broadcasted_iota(jnp.int32, (rows, columns), 0)
    c = lax.broadcasted_iota(jnp.int32, (rows, columns), 1)
    hit = c == column_of(r)
    if keep is not None:
        hit = hit & keep(r)
    return jnp.where(hit, 1.0, 0.0).astype(BF16)


def rms(x):
    return x * lax.rsqrt(jnp.mean(x * x, axis=-1, keepdims=True) + 1e-06)


def finish_pair(s, vst, ones, keys):
    s_lo, s_hi = s[:, :keys], s[:, keys:]
    p_lo = jnp.exp2(s_lo - jnp.max(s_lo, axis=-1, keepdims=True)).astype(BF16)
    p_hi = jnp.exp2(s_hi - jnp.max(s_hi, axis=-1, keepdims=True)).astype(BF16)
    p = jnp.concatenate([p_lo, p_hi], axis=1)
    o = dot(p, jnp.concatenate([vst, ones], axis=1))
    return (o[:, :128] / o[:, 128:]).astype(BF16)


def pipelined(blocks, scores, finish):
    ahead = scores(*blocks[0])
    for n, block in enumerate(blocks):
        now = ahead
        if n + 1 < len(blocks):
            ahead = scores(*blocks[n + 1])
        finish(now, *block)


def kernel(
    video, emb, cond, sgain, sqkv, sout, tgain, tqkv, tout, merge, cgain, cqkv, cout, up,
    recv2, zr,
    vid, wcond, wsq, wso, wtq, wto, wm, wcq, wco, wup,
    sq, skst, svst, ones_s, smix,
    sbuf1, recv1, sbufl, recvl, esend, frecv,
    perm, xt, tq, tkst, tvst, ones_t, tmix,
    sbuf2, cbuf,
    c0, cq, ck, cv, cmix, zs,
    modv, lsem, vsem, osem, ss1, rs1, ss2, rs2, ss3, rs3, ssl, rsl,
):
    clip = lax.axis_index("clip")
    me = lax.axis_index("frame")
    z, x, y = me // 8, lax.rem(me // 2, 4), lax.rem(me, 2)

    def peer(o):
        return lax.rem(z + o[0], 4) * 8 + lax.rem(x + o[1], 4) * 2 + lax.rem(y + o[2], 2)

    barrier = pltpu.get_barrier_semaphore()
    for o in OFFSETS:
        pl.semaphore_signal(barrier, inc=1, device_id=(clip, peer(o)), device_id_type=MESH)

    weights = [
        (cond, wcond), (sqkv, wsq), (sout, wso), (tqkv, wtq), (tout, wto),
        (merge, wm), (cqkv, wcq), (cout, wco), (up, wup),
    ]
    wcopy = [pltpu.make_async_copy(a, b, lsem.at[i]) for i, (a, b) in enumerate(weights)]
    vcopy = [pltpu.make_async_copy(video.at[f], vid.at[f], vsem.at[f]) for f in range(4)]
    vcopy[0].start()
    for i in range(3):
        wcopy[i].start()
    for f in range(1, 4):
        vcopy[f].start()

    lane = lax.broadcasted_iota(jnp.int32, (1, 128), 1)
    lo = jnp.where(lane < HEAD, 1.0, 0.0).astype(F32)
    hi = 1.0 - lo
    ones_s[0:512, :] = jnp.broadcast_to(lo, (512, 128)).astype(BF16)
    ones_s[512:1024, :] = jnp.broadcast_to(hi, (512, 128)).astype(BF16)
    ones_t[0:128, :] = jnp.broadcast_to(lo, (128, 128)).astype(BF16)
    ones_t[128:256, :] = jnp.broadcast_to(hi, (128, 128)).astype(BF16)
    perm[...] = onehot(256, 256, lambda r: (r & 15) * 16 + (r >> 4))
    for h in range(2):
        esend[h] = onehot(
            256, 128,
            lambda r: ((r >> 4) & 7) * 16 + (r >> 7) * 8 + (r & 7),
            lambda r: ((r >> 3) & 1) == h,
        )
        frecv[h] = onehot(128, 256, lambda r: (r & 15) * 16 + h * 8 + (r >> 4))

    wcopy[0].wait()
    e1 = emb[...].astype(BF16).astype(F32)
    e2 = (emb[...] - e1).astype(BF16).astype(F32)
    e3 = emb[...] - e1 - e2
    piece = lax.broadcasted_iota(jnp.int32, (8, 128), 0)
    pieces = jnp.where(piece == 0, e1, jnp.where(piece == 1, e2, jnp.where(piece == 2, e3, 0.0)))
    modv[...] = jnp.sum(dot(pieces.astype(BF16), wcond[...]), axis=0, keepdims=True)
    sg = sgain[...] * (1.0 + modv[:, 0:D])
    shs = modv[:, D : 2 * D]
    tg = tgain[...] * (1.0 + modv[:, 2 * D : 3 * D])
    sht = modv[:, 3 * D : 4 * D]

    wcopy[1].wait()
    wcopy[2].wait()
    for i in range(3, 9):
        wcopy[i].start()

    def send_late(half, o):
        to = peer(o)
        pltpu.make_async_remote_copy(
            src_ref=sbufl.at[half, to],
            dst_ref=recvl.at[half, me],
            send_sem=ssl,
            recv_sem=rsl.at[half],
            device_id=(clip, to),
            device_id_type=MESH,
        ).start()

    def frame_step(f, last):
        pltpu.make_async_copy(video.at[f], vid.at[f], vsem.at[f]).wait()
        xf = vid[f].astype(F32)
        normed = (rms(xf) * sg + shs).astype(BF16)
        sq[...] = (dot(normed, wsq[:, 0:D]) * QSCALE).astype(BF16)
        for p in range(4):
            k2 = dot(normed, wsq[:, D + p * 128 : D + (p + 1) * 128])
            skst[p, 0:512] = (k2 * lo).astype(BF16)
            skst[p, 512:1024] = (k2 * hi).astype(BF16)
            v2 = dot(normed, wsq[:, 2 * D + p * 128 : 2 * D + (p + 1) * 128])
            svst[p, 0:512] = (v2 * lo).astype(BF16)
            svst[p, 512:1024] = (v2 * hi).astype(BF16)

        if not last:

            @pl.when(f == 0)
            def _():
                pl.semaphore_wait(barrier, len(OFFSETS))

        def rows_of(dz):
            return pl.ds(pl.multiple_of(lax.rem(z + dz, 4) * 128, 128), 128)

        def scores(dz, p):
            return dot_t(sq[rows_of(dz), p * 128 : (p + 1) * 128], skst[p])

        def finish(v, dz, p):
            rows = rows_of(dz)
            smix[rows, p * 128 : (p + 1) * 128] = finish_pair(v, svst[p], ones_s[...], 512)
            if p < 3:
                return
            fine1 = (vid[f, rows, :].astype(F32) + dot(smix[rows, :], wso[...])).astype(BF16)
            if last:
                halves = dot(esend[0], fine1[:, :256]) + dot(esend[1], fine1[:, 256:])
                halves = halves.astype(BF16).reshape(2, 8, 16, 256)
                devices = pl.ds(lax.rem(z + dz, 4) * 8, 8)
                sbufl[0, devices] = halves[0]
                sbufl[1, devices] = halves[1]
                if dz == 0:
                    recvl[0, me] = sbufl[0, me]
                    recvl[1, me] = sbufl[1, me]
                for o in OFFSETS:
                    if o[0] == dz:
                        send_late(0, o)
                return
            sbuf1[f, rows, :] = fine1
            if dz == 0:
                own = pl.ds(pl.multiple_of(me * 16, 16), 16)
                recv1[f * GROUP + me] = sbuf1[f, own, :]
            for o in OFFSETS:
                if o[0] == dz:
                    to = peer(o)
                    pltpu.make_async_remote_copy(
                        src_ref=sbuf1.at[f, pl.ds(pl.multiple_of(to * 16, 16), 16), :],
                        dst_ref=recv1.at[f * GROUP + me],
                        send_sem=ss1,
                        recv_sem=rs1.at[f],
                        device_id=(clip, to),
                        device_id_type=MESH,
                    ).start()

        pipelined([(dz, p) for dz in (2, 1, 3, 0) for p in range(4)], scores, finish)
        if last:
            for o in OFFSETS:
                send_late(1, o)

    def early_frame(f, carry):
        frame_step(f, False)
        return carry

    lax.fori_loop(0, 3, early_frame, 0)
    frame_step(3, True)

    wcopy[3].wait()
    wcopy[4].wait()

    def project(yg, tokens, base):
        count = yg.shape[0] // 16
        frames = pl.ds(pl.multiple_of(base, 16), 16)
        high = pl.ds(pl.multiple_of(128 + base, 16), 16)
        xt[tokens, frames, :] = yg.astype(BF16).reshape(count, 16, D)
        normed = (rms(yg) * tg + sht).astype(BF16)
        q = dot(normed, wtq[:, 0:D]) * QSCALE
        tq[tokens, frames, :] = q.astype(BF16).reshape(count, 16, D)
        for p in range(4):
            k2 = dot(normed, wtq[:, D + p * 128 : D + (p + 1) * 128])
            tkst[tokens, p, frames, :] = (k2 * lo).astype(BF16).reshape(count, 16, 128)
            tkst[tokens, p, high, :] = (k2 * hi).astype(BF16).reshape(count, 16, 128)
            v2 = dot(normed, wtq[:, 2 * D + p * 128 : 2 * D + (p + 1) * 128])
            tvst[tokens, p, frames, :] = (v2 * lo).astype(BF16).reshape(count, 16, 128)
            tvst[tokens, p, high, :] = (v2 * hi).astype(BF16).reshape(count, 16, 128)

    def group_step(j, carry):
        pltpu.make_async_copy(recv1.at[pl.ds(0, 31)], recv1.at[pl.ds(0, 31)], rs1.at[j]).wait()
        for sb in range(2):
            base = j * GROUP + sb * 16
            frames = pl.ds(pl.multiple_of(base, 16), 16)
            project(dot(perm[...], recv1[frames].reshape(256, D)), slice(0, 16), base)
        return carry

    def late_group(half):
        pltpu.make_async_copy(
            recvl.at[half, pl.ds(0, 31)], recvl.at[half, pl.ds(0, 31)], rsl.at[half]
        ).wait()
        for sb in range(2):
            got = recvl[half, sb * 16 : (sb + 1) * 16].reshape(256, 256)
            yg = jnp.concatenate([dot(frecv[0], got), dot(frecv[1], got)], axis=1)
            project(yg, slice(half * 8, half * 8 + 8), 3 * GROUP + sb * 16)

    lax.fori_loop(0, 3, group_step, 0)
    late_group(0)

    def token_step(c, carry):
        @pl.when(c == 2)
        def _():
            late_group(1)

        def scores(q, p):
            return dot_t(tq[c * 4 + q, :, p * 128 : (p + 1) * 128], tkst[c * 4 + q, p])

        def finish(v, q, p):
            tmix[q, :, p * 128 : (p + 1) * 128] = finish_pair(
                v, tvst[c * 4 + q, p], ones_t[...], 128
            )

        pipelined([(q, p) for q in range(4) for p in range(4)], scores, finish)
        for q in range(4):
            tmix[q] = (xt[c * 4 + q].astype(F32) + dot(tmix[q], wto[...])).astype(BF16)
        for sb in range(2):
            fg = jnp.concatenate(
                [
                    tmix[q, j * GROUP + sb * 16 : j * GROUP + (sb + 1) * 16, :]
                    for j in range(4) for q in range(4)
                ],
                axis=0,
            )
            sbuf2[c, sb * 16 : (sb + 1) * 16] = dot(perm[...], fg).astype(BF16).reshape(16, 16, D)
        pltpu.make_async_copy(sbuf2.at[c, me], recv2.at[c, me], osem.at[c]).start()
        for o in OFFSETS:
            to = peer(o)
            pltpu.make_async_remote_copy(
                src_ref=sbuf2.at[c, to],
                dst_ref=recv2.at[c, me],
                send_sem=ss2,
                recv_sem=rs2,
                device_id=(clip, to),
                device_id_type=MESH,
            ).start()
        for d in range(2):
            for q in range(4):
                for jh in range(2):
                    j = 2 * jh + d
                    cbuf[
                        pl.ds(pl.multiple_of(c * 64 + jh * 32, 32), 32),
                        (d * 4 + q) * D : (d * 4 + q + 1) * D,
                    ] = tmix[q, j * GROUP : (j + 1) * GROUP, :]
        return carry

    lax.fori_loop(0, 4, token_step, 0)
    mine = pl.ds(pl.multiple_of(me * 16, 16), 16)

    for i in range(5, 9):
        wcopy[i].wait()
    c0[...] = dot(cbuf[...], wm[...]).astype(BF16)
    normed = (rms(c0[...].astype(F32)) * cgain[...]).astype(BF16)
    cq[...] = (dot(normed, wcq[:, 0:DC]) * QSCALE).astype(BF16)
    ck[...] = dot(normed, wcq[:, DC : 2 * DC]).astype(BF16)
    cv[...] = dot(normed, wcq[:, 2 * DC : 3 * DC]).astype(BF16)
    lane4 = lax.broadcasted_iota(jnp.int32, (64, 256), 1) >> 6
    block4 = jnp.concatenate(
        [jnp.where(lane4 == h, 1.0, 0.0).astype(BF16) for h in range(4)], axis=0
    )
    low = lax.broadcasted_iota(jnp.int32, (64, 128), 1) < HEAD

    def cell_scores(b, hg):
        rows, lanes = slice(b * 64, (b + 1) * 64), slice(hg * 256, (hg + 1) * 256)
        return dot_t(cq[rows, lanes], jnp.concatenate([ck[rows, lanes]] * 4, axis=0) * block4)

    def cell_finish(s, b, hg):
        rows, lanes = slice(b * 64, (b + 1) * 64), slice(hg * 256, (hg + 1) * 256)
        parts = []
        for half in range(2):
            sh = s[:, half * 128 : (half + 1) * 128]
            m_lo = jnp.max(jnp.where(low, sh, -jnp.inf), axis=-1, keepdims=True)
            m_hi = jnp.max(jnp.where(low, -jnp.inf, sh), axis=-1, keepdims=True)
            parts.append(jnp.exp2(sh - jnp.where(low, m_lo, m_hi)).astype(BF16))
        p = jnp.concatenate(parts, axis=1)
        o = dot(p, jnp.concatenate([cv[rows, lanes]] * 4, axis=0) * block4)
        cmix[rows, lanes] = (o / dot(p, block4)).astype(BF16)

    pipelined([(b, hg) for b in range(4) for hg in range(4)], cell_scores, cell_finish)
    coarse1 = (c0[...].astype(F32) + dot(cmix[...], wco[...])).astype(BF16)
    upped = dot(coarse1, wup[...]).astype(BF16)

    def pick(half):
        r = lax.broadcasted_iota(jnp.int32, (512, 256), 0)
        c = lax.broadcasted_iota(jnp.int32, (512, 256), 1)
        hit = (c == (r & 3) * 64 + ((r >> 2) & 1) * 32 + (r >> 4)) & (((r >> 3) & 1) == half)
        return jnp.where(hit, 1.0, 0.0).astype(BF16)

    zs[...] = (dot(pick(0), upped[:, :256]) + dot(pick(1), upped[:, 256:])).astype(BF16)
    own_z = pltpu.make_async_copy(zs.at[mine], zr.at[mine], osem.at[4])
    own_z.start()
    for o in OFFSETS:
        to = peer(o)
        pltpu.make_async_remote_copy(
            src_ref=zs.at[pl.ds(pl.multiple_of(to * 16, 16), 16), :],
            dst_ref=zr.at[mine, :],
            send_sem=ss3,
            recv_sem=rs3,
            device_id=(clip, to),
            device_id_type=MESH,
        ).start()

    pltpu.make_async_copy(recv2.at[:, pl.ds(0, 31)], recv2.at[:, pl.ds(0, 31)], rs2).wait()
    pltpu.make_async_copy(zr.at[pl.ds(0, 496)], zr.at[pl.ds(0, 496)], rs3).wait()
    pltpu.make_async_copy(sbuf1.at[:, pl.ds(0, 496), :], sbuf1.at[:, pl.ds(0, 496), :], ss1).wait()
    pltpu.make_async_copy(sbufl.at[:, pl.ds(0, 31)], sbufl.at[:, pl.ds(0, 31)], ssl).wait()
    pltpu.make_async_copy(sbuf2.at[:, pl.ds(0, 31)], sbuf2.at[:, pl.ds(0, 31)], ss2).wait()
    pltpu.make_async_copy(zs.at[pl.ds(0, 496)], zs.at[pl.ds(0, 496)], ss3).wait()
    for c in range(4):
        pltpu.make_async_copy(sbuf2.at[c, me], recv2.at[c, me], osem.at[c]).wait()
    own_z.wait()


def combine(fine, coarse, out, got, zin, res, perm, spread, isem, osem):
    def part(sb):
        return pl.ds(sb * 4, 4)

    zcopy = pltpu.make_async_copy(coarse, zin, isem.at[8])
    zcopy.start()
    icopy = [
        pltpu.make_async_copy(fine.at[:, part(sb)], got.at[:, part(sb)], isem.at[sb])
        for sb in range(8)
    ]
    for cp in icopy:
        cp.start()
    perm[...] = onehot(
        256, 256, lambda r: ((r >> 2) & 3) * 64 + ((r >> 4) & 3) * 16 + (r >> 6) * 4 + (r & 3)
    )
    for half in range(2):
        spread[half] = onehot(
            256, 64,
            lambda r: ((r >> 4) & 3) * 16 + half * 8 + (r >> 7) * 4 + ((r >> 2) & 3),
        )
    zcopy.wait()
    ocopy = []
    for sb in range(8):
        icopy[sb].wait()
        rows = slice(sb * 64, (sb + 1) * 64)
        cells = jnp.concatenate([got[c, part(sb)].reshape(64, D) for c in range(4)], axis=0)
        for half in range(2):
            lanes = slice(half * 256, (half + 1) * 256)
            total = dot(perm[...], cells[:, lanes]) + dot(spread[half], zin[rows, :])
            for j in range(4):
                res[j, rows, lanes] = total[j * 64 : (j + 1) * 64].astype(BF16)
        cp = pltpu.make_async_copy(
            res.at[:, pl.ds(sb * 64, 64), :], out.at[:, pl.ds(sb * 64, 64), :], osem.at[sb]
        )
        cp.start()
        ocopy.append(cp)
    for cp in ocopy:
        cp.wait()


def body(
    video, timestep, cond_weight, spatial_gain, spatial_qkv, spatial_out, temporal_gain,
    temporal_qkv, temporal_out, merge_weight, coarse_gain, coarse_qkv, coarse_out, up_weight,
):
    counter = jnp.arange(FREQ, dtype=F32)
    frequency = jnp.exp(counter * (-math.log(10000.0) / FREQ))
    angles = timestep.astype(F32)[0] * frequency
    emb = jnp.concatenate([jnp.sin(angles), jnp.cos(angles)])[None]
    any_, vm = pl.BlockSpec(memory_space=pl.ANY), pl.BlockSpec(memory_space=pltpu.VMEM)
    b = lambda *shape: pltpu.VMEM(shape, BF16)
    fine, coarse = pl.pallas_call(
        kernel,
        name="denoise",
        out_shape=[
            jax.ShapeDtypeStruct((4, GROUP, 16, D), BF16),
            jax.ShapeDtypeStruct((512, 256), BF16),
        ],
        in_specs=[any_, vm, any_, vm, any_, any_, vm, any_, any_, any_, vm, any_, any_, any_],
        out_specs=[any_, any_],
        scratch_shapes=[
            b(4, 512, D), b(128, 2048), b(D, 3 * D), b(D, D), b(D, 3 * D), b(D, D),
            b(8 * D, DC), b(DC, 3 * DC), b(DC, DC), b(DC, D),
            b(512, D), b(4, 1024, 128), b(4, 1024, 128), b(1024, 128), b(512, D),
            b(3, 512, D), b(96, 16, D), b(2, GROUP, 16, 256), b(2, GROUP, 16, 256),
            b(2, 256, 128), b(2, 128, 256),
            b(256, 256), b(16, 128, D), b(16, 128, D), b(16, 4, 256, 128),
            b(16, 4, 256, 128), b(256, 128), b(4, 128, D),
            b(4, 32, 16, D), b(256, 8 * D),
            b(256, DC), b(256, DC), b(256, DC), b(256, DC), b(256, DC), b(512, 256),
            pltpu.VMEM((1, 4 * D), F32),
            pltpu.SemaphoreType.DMA((9,)), pltpu.SemaphoreType.DMA((4,)),
            pltpu.SemaphoreType.DMA((8,)),
            pltpu.SemaphoreType.DMA, pltpu.SemaphoreType.DMA((3,)),
        ] + [pltpu.SemaphoreType.DMA] * 5 + [pltpu.SemaphoreType.DMA((2,))],
        compiler_params=pltpu.CompilerParams(
            collective_id=0, has_side_effects=True, vmem_limit_bytes=67_000_000
        ),
    )(
        video, emb, cond_weight, spatial_gain[None], spatial_qkv, spatial_out,
        temporal_gain[None], temporal_qkv, temporal_out, merge_weight, coarse_gain[None],
        coarse_qkv, coarse_out, up_weight,
    )
    return pl.pallas_call(
        combine,
        name="combine",
        out_shape=jax.ShapeDtypeStruct(video.shape, BF16),
        in_specs=[any_, any_],
        out_specs=any_,
        scratch_shapes=[
            b(4, GROUP, 16, D), b(512, 256), b(4, 512, D), b(256, 256), b(2, 256, 64),
            pltpu.SemaphoreType.DMA((9,)), pltpu.SemaphoreType.DMA((8,)),
        ],
    )(fine, coarse)


def solution(mesh):
    return jax.shard_map(
        body,
        mesh=mesh,
        in_specs=(P(("clip", "frame"), None, None), P("clip")) + (P(),) * 12,
        out_specs=P(("clip", "frame"), None, None),
        check_vma=False,
    )
```

```python
import math

import jax
import jax.numpy as jnp
from jax import lax
from jax.experimental import pallas as pl
from jax.experimental.pallas import tpu as pltpu
from jax.sharding import PartitionSpec as P

D = 512
DC = 1024
HEAD = 64
FREQ = 64
GROUP = 32
MESH = pl.DeviceIdType.MESH
F32 = jnp.float32
BF16 = jnp.bfloat16
QSCALE = math.log2(math.e) / math.sqrt(HEAD)

OFFSETS = sorted(
    [(a, b, d) for a in range(4) for b in range(4) for d in range(2) if (a, b, d) != (0, 0, 0)],
    key=lambda o: -(min(o[0], 4 - o[0]) + min(o[1], 4 - o[1]) + o[2]),
)


def dot(a, b):
    return jnp.dot(a, b, preferred_element_type=F32)


def dot_t(a, b):
    return lax.dot_general(a, b, (((1,), (1,)), ((), ())), preferred_element_type=F32)


def onehot(rows, columns, column_of, keep=None):
    r = lax.broadcasted_iota(jnp.int32, (rows, columns), 0)
    c = lax.broadcasted_iota(jnp.int32, (rows, columns), 1)
    hit = c == column_of(r)
    if keep is not None:
        hit = hit & keep(r)
    return jnp.where(hit, 1.0, 0.0).astype(BF16)


def rms(x):
    return x * lax.rsqrt(jnp.mean(x * x, axis=-1, keepdims=True) + 1e-06)


def finish_pair(s, vst, ones, keys):
    s_lo, s_hi = s[:, :keys], s[:, keys:]
    p_lo = jnp.exp2(s_lo - jnp.max(s_lo, axis=-1, keepdims=True)).astype(BF16)
    p_hi = jnp.exp2(s_hi - jnp.max(s_hi, axis=-1, keepdims=True)).astype(BF16)
    p = jnp.concatenate([p_lo, p_hi], axis=1)
    o = dot(p, jnp.concatenate([vst, ones], axis=1))
    return (o[:, :128] / o[:, 128:]).astype(BF16)


def pipelined(blocks, scores, finish):
    ahead = scores(*blocks[0])
    for n, block in enumerate(blocks):
        now = ahead
        if n + 1 < len(blocks):
            ahead = scores(*blocks[n + 1])
        finish(now, *block)


def kernel(
    video, emb, cond, sgain, sqkv, sout, tgain, tqkv, tout, merge, cgain, cqkv, cout, up,
    recv2, zr,
    vid, wcond, wsq, wso, wtq, wto, wm, wcq, wco, wup,
    sq, skst, svst, ones_s, smix,
    sbuf1, recv1, sbufl, recvl, esend, frecv,
    perm, xt, tq, tkst, tvst, ones_t, tmix,
    sbuf2, cbuf,
    c0, cq, ck, cv, cmix, zs,
    modv, lsem, vsem, osem, ss1, rs1, ss2, rs2, ss3, rs3, ssl, rsl,
):
    clip = lax.axis_index("clip")
    me = lax.axis_index("frame")
    z, x, y = me // 8, lax.rem(me // 2, 4), lax.rem(me, 2)

    def peer(o):
        return lax.rem(z + o[0], 4) * 8 + lax.rem(x + o[1], 4) * 2 + lax.rem(y + o[2], 2)

    barrier = pltpu.get_barrier_semaphore()
    for o in OFFSETS:
        pl.semaphore_signal(barrier, inc=1, device_id=(clip, peer(o)), device_id_type=MESH)

    weights = [
        (cond, wcond), (sqkv, wsq), (sout, wso), (tqkv, wtq), (tout, wto),
        (merge, wm), (cqkv, wcq), (cout, wco), (up, wup),
    ]
    wcopy = [pltpu.make_async_copy(a, b, lsem.at[i]) for i, (a, b) in enumerate(weights)]
    vcopy = [pltpu.make_async_copy(video.at[f], vid.at[f], vsem.at[f]) for f in range(4)]
    vcopy[0].start()
    for i in range(3):
        wcopy[i].start()
    for f in range(1, 4):
        vcopy[f].start()

    lane = lax.broadcasted_iota(jnp.int32, (1, 128), 1)
    lo = jnp.where(lane < HEAD, 1.0, 0.0).astype(F32)
    hi = 1.0 - lo
    ones_s[0:512, :] = jnp.broadcast_to(lo, (512, 128)).astype(BF16)
    ones_s[512:1024, :] = jnp.broadcast_to(hi, (512, 128)).astype(BF16)
    ones_t[0:128, :] = jnp.broadcast_to(lo, (128, 128)).astype(BF16)
    ones_t[128:256, :] = jnp.broadcast_to(hi, (128, 128)).astype(BF16)
    perm[...] = onehot(256, 256, lambda r: (r & 15) * 16 + (r >> 4))
    for h in range(2):
        esend[h] = onehot(
            256, 128,
            lambda r: ((r >> 4) & 7) * 16 + (r >> 7) * 8 + (r & 7),
            lambda r: ((r >> 3) & 1) == h,
        )
        frecv[h] = onehot(128, 256, lambda r: (r & 15) * 16 + h * 8 + (r >> 4))

    wcopy[0].wait()
    e1 = emb[...].astype(BF16).astype(F32)
    e2 = (emb[...] - e1).astype(BF16).astype(F32)
    e3 = emb[...] - e1 - e2
    piece = lax.broadcasted_iota(jnp.int32, (8, 128), 0)
    pieces = jnp.where(piece == 0, e1, jnp.where(piece == 1, e2, jnp.where(piece == 2, e3, 0.0)))
    modv[...] = jnp.sum(dot(pieces.astype(BF16), wcond[...]), axis=0, keepdims=True)
    sg = sgain[...] * (1.0 + modv[:, 0:D])
    shs = modv[:, D : 2 * D]
    tg = tgain[...] * (1.0 + modv[:, 2 * D : 3 * D])
    sht = modv[:, 3 * D : 4 * D]

    wcopy[1].wait()
    wcopy[2].wait()
    for i in range(3, 9):
        wcopy[i].start()

    def send_late(half, o):
        to = peer(o)
        pltpu.make_async_remote_copy(
            src_ref=sbufl.at[half, to],
            dst_ref=recvl.at[half, me],
            send_sem=ssl,
            recv_sem=rsl.at[half],
            device_id=(clip, to),
            device_id_type=MESH,
        ).start()

    def frame_step(f, last):
        pltpu.make_async_copy(video.at[f], vid.at[f], vsem.at[f]).wait()
        xf = vid[f].astype(F32)
        normed = (rms(xf) * sg + shs).astype(BF16)
        sq[...] = (dot(normed, wsq[:, 0:D]) * QSCALE).astype(BF16)
        for p in range(4):
            k2 = dot(normed, wsq[:, D + p * 128 : D + (p + 1) * 128])
            skst[p, 0:512] = (k2 * lo).astype(BF16)
            skst[p, 512:1024] = (k2 * hi).astype(BF16)
            v2 = dot(normed, wsq[:, 2 * D + p * 128 : 2 * D + (p + 1) * 128])
            svst[p, 0:512] = (v2 * lo).astype(BF16)
            svst[p, 512:1024] = (v2 * hi).astype(BF16)

        if not last:

            @pl.when(f == 0)
            def _():
                pl.semaphore_wait(barrier, len(OFFSETS))

        def rows_of(dz):
            return pl.ds(pl.multiple_of(lax.rem(z + dz, 4) * 128, 128), 128)

        def scores(dz, p):
            return dot_t(sq[rows_of(dz), p * 128 : (p + 1) * 128], skst[p])

        def finish(v, dz, p):
            rows = rows_of(dz)
            smix[rows, p * 128 : (p + 1) * 128] = finish_pair(v, svst[p], ones_s[...], 512)
            if p < 3:
                return
            fine1 = (vid[f, rows, :].astype(F32) + dot(smix[rows, :], wso[...])).astype(BF16)
            if last:
                halves = dot(esend[0], fine1[:, :256]) + dot(esend[1], fine1[:, 256:])
                halves = halves.astype(BF16).reshape(2, 8, 16, 256)
                devices = pl.ds(lax.rem(z + dz, 4) * 8, 8)
                sbufl[0, devices] = halves[0]
                sbufl[1, devices] = halves[1]
                if dz == 0:
                    recvl[0, me] = sbufl[0, me]
                    recvl[1, me] = sbufl[1, me]
                for o in OFFSETS:
                    if o[0] == dz:
                        send_late(0, o)
                return
            sbuf1[f, rows, :] = fine1
            if dz == 0:
                own = pl.ds(pl.multiple_of(me * 16, 16), 16)
                recv1[f * GROUP + me] = sbuf1[f, own, :]
            for o in OFFSETS:
                if o[0] == dz:
                    to = peer(o)
                    pltpu.make_async_remote_copy(
                        src_ref=sbuf1.at[f, pl.ds(pl.multiple_of(to * 16, 16), 16), :],
                        dst_ref=recv1.at[f * GROUP + me],
                        send_sem=ss1,
                        recv_sem=rs1.at[f],
                        device_id=(clip, to),
                        device_id_type=MESH,
                    ).start()

        pipelined([(dz, p) for dz in (2, 1, 3, 0) for p in range(4)], scores, finish)

    def early_frame(f, carry):
        frame_step(f, False)
        return carry

    lax.fori_loop(0, 3, early_frame, 0)
    frame_step(3, True)

    wcopy[3].wait()
    wcopy[4].wait()

    def project(yg, tokens, base):
        count = yg.shape[0] // 16
        frames = pl.ds(pl.multiple_of(base, 16), 16)
        high = pl.ds(pl.multiple_of(128 + base, 16), 16)
        xt[tokens, frames, :] = yg.astype(BF16).reshape(count, 16, D)
        normed = (rms(yg) * tg + sht).astype(BF16)
        q = dot(normed, wtq[:, 0:D]) * QSCALE
        tq[tokens, frames, :] = q.astype(BF16).reshape(count, 16, D)
        for p in range(4):
            k2 = dot(normed, wtq[:, D + p * 128 : D + (p + 1) * 128])
            tkst[tokens, p, frames, :] = (k2 * lo).astype(BF16).reshape(count, 16, 128)
            tkst[tokens, p, high, :] = (k2 * hi).astype(BF16).reshape(count, 16, 128)
            v2 = dot(normed, wtq[:, 2 * D + p * 128 : 2 * D + (p + 1) * 128])
            tvst[tokens, p, frames, :] = (v2 * lo).astype(BF16).reshape(count, 16, 128)
            tvst[tokens, p, high, :] = (v2 * hi).astype(BF16).reshape(count, 16, 128)

    def group_step(j, carry):
        pltpu.make_async_copy(recv1.at[pl.ds(0, 31)], recv1.at[pl.ds(0, 31)], rs1.at[j]).wait()

        @pl.when(j == 2)
        def _():
            for o in OFFSETS:
                send_late(1, o)

        for sb in range(2):
            base = j * GROUP + sb * 16
            frames = pl.ds(pl.multiple_of(base, 16), 16)
            project(dot(perm[...], recv1[frames].reshape(256, D)), slice(0, 16), base)
        return carry

    def late_group(half):
        pltpu.make_async_copy(
            recvl.at[half, pl.ds(0, 31)], recvl.at[half, pl.ds(0, 31)], rsl.at[half]
        ).wait()
        for sb in range(2):
            got = recvl[half, sb * 16 : (sb + 1) * 16].reshape(256, 256)
            yg = jnp.concatenate([dot(frecv[0], got), dot(frecv[1], got)], axis=1)
            project(yg, slice(half * 8, half * 8 + 8), 3 * GROUP + sb * 16)

    lax.fori_loop(0, 3, group_step, 0)
    late_group(0)

    def token_step(c, carry):
        @pl.when(c == 2)
        def _():
            late_group(1)

        def scores(q, p):
            return dot_t(tq[c * 4 + q, :, p * 128 : (p + 1) * 128], tkst[c * 4 + q, p])

        def finish(v, q, p):
            tmix[q, :, p * 128 : (p + 1) * 128] = finish_pair(
                v, tvst[c * 4 + q, p], ones_t[...], 128
            )

        pipelined([(q, p) for q in range(4) for p in range(4)], scores, finish)
        for q in range(4):
            tmix[q] = (xt[c * 4 + q].astype(F32) + dot(tmix[q], wto[...])).astype(BF16)
        for sb in range(2):
            fg = jnp.concatenate(
                [
                    tmix[q, j * GROUP + sb * 16 : j * GROUP + (sb + 1) * 16, :]
                    for j in range(4) for q in range(4)
                ],
                axis=0,
            )
            sbuf2[c, sb * 16 : (sb + 1) * 16] = dot(perm[...], fg).astype(BF16).reshape(16, 16, D)
        pltpu.make_async_copy(sbuf2.at[c, me], recv2.at[c, me], osem.at[c]).start()
        for o in OFFSETS:
            to = peer(o)
            pltpu.make_async_remote_copy(
                src_ref=sbuf2.at[c, to],
                dst_ref=recv2.at[c, me],
                send_sem=ss2,
                recv_sem=rs2,
                device_id=(clip, to),
                device_id_type=MESH,
            ).start()
        for d in range(2):
            for q in range(4):
                for jh in range(2):
                    j = 2 * jh + d
                    cbuf[
                        pl.ds(pl.multiple_of(c * 64 + jh * 32, 32), 32),
                        (d * 4 + q) * D : (d * 4 + q + 1) * D,
                    ] = tmix[q, j * GROUP : (j + 1) * GROUP, :]
        return carry

    lax.fori_loop(0, 4, token_step, 0)
    mine = pl.ds(pl.multiple_of(me * 16, 16), 16)

    for i in range(5, 9):
        wcopy[i].wait()
    c0[...] = dot(cbuf[...], wm[...]).astype(BF16)
    normed = (rms(c0[...].astype(F32)) * cgain[...]).astype(BF16)
    cq[...] = (dot(normed, wcq[:, 0:DC]) * QSCALE).astype(BF16)
    ck[...] = dot(normed, wcq[:, DC : 2 * DC]).astype(BF16)
    cv[...] = dot(normed, wcq[:, 2 * DC : 3 * DC]).astype(BF16)
    lane4 = lax.broadcasted_iota(jnp.int32, (64, 256), 1) >> 6
    block4 = jnp.concatenate(
        [jnp.where(lane4 == h, 1.0, 0.0).astype(BF16) for h in range(4)], axis=0
    )
    low = lax.broadcasted_iota(jnp.int32, (64, 128), 1) < HEAD

    def cell_scores(b, hg):
        rows, lanes = slice(b * 64, (b + 1) * 64), slice(hg * 256, (hg + 1) * 256)
        return dot_t(cq[rows, lanes], jnp.concatenate([ck[rows, lanes]] * 4, axis=0) * block4)

    def cell_finish(s, b, hg):
        rows, lanes = slice(b * 64, (b + 1) * 64), slice(hg * 256, (hg + 1) * 256)
        parts = []
        for half in range(2):
            sh = s[:, half * 128 : (half + 1) * 128]
            m_lo = jnp.max(jnp.where(low, sh, -jnp.inf), axis=-1, keepdims=True)
            m_hi = jnp.max(jnp.where(low, -jnp.inf, sh), axis=-1, keepdims=True)
            parts.append(jnp.exp2(sh - jnp.where(low, m_lo, m_hi)).astype(BF16))
        p = jnp.concatenate(parts, axis=1)
        o = dot(p, jnp.concatenate([cv[rows, lanes]] * 4, axis=0) * block4)
        cmix[rows, lanes] = (o / dot(p, block4)).astype(BF16)

    pipelined([(b, hg) for b in range(4) for hg in range(4)], cell_scores, cell_finish)
    coarse1 = (c0[...].astype(F32) + dot(cmix[...], wco[...])).astype(BF16)
    upped = dot(coarse1, wup[...]).astype(BF16)

    def pick(half):
        r = lax.broadcasted_iota(jnp.int32, (512, 256), 0)
        c = lax.broadcasted_iota(jnp.int32, (512, 256), 1)
        hit = (c == (r & 3) * 64 + ((r >> 2) & 1) * 32 + (r >> 4)) & (((r >> 3) & 1) == half)
        return jnp.where(hit, 1.0, 0.0).astype(BF16)

    zs[...] = (dot(pick(0), upped[:, :256]) + dot(pick(1), upped[:, 256:])).astype(BF16)
    own_z = pltpu.make_async_copy(zs.at[mine], zr.at[mine], osem.at[4])
    own_z.start()
    for o in OFFSETS:
        to = peer(o)
        pltpu.make_async_remote_copy(
            src_ref=zs.at[pl.ds(pl.multiple_of(to * 16, 16), 16), :],
            dst_ref=zr.at[mine, :],
            send_sem=ss3,
            recv_sem=rs3,
            device_id=(clip, to),
            device_id_type=MESH,
        ).start()

    pltpu.make_async_copy(recv2.at[:, pl.ds(0, 31)], recv2.at[:, pl.ds(0, 31)], rs2).wait()
    pltpu.make_async_copy(zr.at[pl.ds(0, 496)], zr.at[pl.ds(0, 496)], rs3).wait()
    pltpu.make_async_copy(sbuf1.at[:, pl.ds(0, 496), :], sbuf1.at[:, pl.ds(0, 496), :], ss1).wait()
    pltpu.make_async_copy(sbufl.at[:, pl.ds(0, 31)], sbufl.at[:, pl.ds(0, 31)], ssl).wait()
    pltpu.make_async_copy(sbuf2.at[:, pl.ds(0, 31)], sbuf2.at[:, pl.ds(0, 31)], ss2).wait()
    pltpu.make_async_copy(zs.at[pl.ds(0, 496)], zs.at[pl.ds(0, 496)], ss3).wait()
    for c in range(4):
        pltpu.make_async_copy(sbuf2.at[c, me], recv2.at[c, me], osem.at[c]).wait()
    own_z.wait()


def combine(fine, coarse, out, got, zin, res, perm, spread, isem, osem):
    def part(sb):
        return pl.ds(sb * 4, 4)

    zcopy = pltpu.make_async_copy(coarse, zin, isem.at[8])
    zcopy.start()
    icopy = [
        pltpu.make_async_copy(fine.at[:, part(sb)], got.at[:, part(sb)], isem.at[sb])
        for sb in range(8)
    ]
    for cp in icopy:
        cp.start()
    perm[...] = onehot(
        256, 256, lambda r: ((r >> 2) & 3) * 64 + ((r >> 4) & 3) * 16 + (r >> 6) * 4 + (r & 3)
    )
    for half in range(2):
        spread[half] = onehot(
            256, 64,
            lambda r: ((r >> 4) & 3) * 16 + half * 8 + (r >> 7) * 4 + ((r >> 2) & 3),
        )
    zcopy.wait()
    ocopy = []
    for sb in range(8):
        icopy[sb].wait()
        rows = slice(sb * 64, (sb + 1) * 64)
        cells = jnp.concatenate([got[c, part(sb)].reshape(64, D) for c in range(4)], axis=0)
        for half in range(2):
            lanes = slice(half * 256, (half + 1) * 256)
            total = dot(perm[...], cells[:, lanes]) + dot(spread[half], zin[rows, :])
            for j in range(4):
                res[j, rows, lanes] = total[j * 64 : (j + 1) * 64].astype(BF16)
        cp = pltpu.make_async_copy(
            res.at[:, pl.ds(sb * 64, 64), :], out.at[:, pl.ds(sb * 64, 64), :], osem.at[sb]
        )
        cp.start()
        ocopy.append(cp)
    for cp in ocopy:
        cp.wait()


def body(
    video, timestep, cond_weight, spatial_gain, spatial_qkv, spatial_out, temporal_gain,
    temporal_qkv, temporal_out, merge_weight, coarse_gain, coarse_qkv, coarse_out, up_weight,
):
    counter = jnp.arange(FREQ, dtype=F32)
    frequency = jnp.exp(counter * (-math.log(10000.0) / FREQ))
    angles = timestep.astype(F32)[0] * frequency
    emb = jnp.concatenate([jnp.sin(angles), jnp.cos(angles)])[None]
    any_, vm = pl.BlockSpec(memory_space=pl.ANY), pl.BlockSpec(memory_space=pltpu.VMEM)
    b = lambda *shape: pltpu.VMEM(shape, BF16)
    fine, coarse = pl.pallas_call(
        kernel,
        name="denoise",
        out_shape=[
            jax.ShapeDtypeStruct((4, GROUP, 16, D), BF16),
            jax.ShapeDtypeStruct((512, 256), BF16),
        ],
        in_specs=[any_, vm, any_, vm, any_, any_, vm, any_, any_, any_, vm, any_, any_, any_],
        out_specs=[any_, any_],
        scratch_shapes=[
            b(4, 512, D), b(128, 2048), b(D, 3 * D), b(D, D), b(D, 3 * D), b(D, D),
            b(8 * D, DC), b(DC, 3 * DC), b(DC, DC), b(DC, D),
            b(512, D), b(4, 1024, 128), b(4, 1024, 128), b(1024, 128), b(512, D),
            b(3, 512, D), b(96, 16, D), b(2, GROUP, 16, 256), b(2, GROUP, 16, 256),
            b(2, 256, 128), b(2, 128, 256),
            b(256, 256), b(16, 128, D), b(16, 128, D), b(16, 4, 256, 128),
            b(16, 4, 256, 128), b(256, 128), b(4, 128, D),
            b(4, 32, 16, D), b(256, 8 * D),
            b(256, DC), b(256, DC), b(256, DC), b(256, DC), b(256, DC), b(512, 256),
            pltpu.VMEM((1, 4 * D), F32),
            pltpu.SemaphoreType.DMA((9,)), pltpu.SemaphoreType.DMA((4,)),
            pltpu.SemaphoreType.DMA((8,)),
            pltpu.SemaphoreType.DMA, pltpu.SemaphoreType.DMA((3,)),
        ] + [pltpu.SemaphoreType.DMA] * 5 + [pltpu.SemaphoreType.DMA((2,))],
        compiler_params=pltpu.CompilerParams(
            collective_id=0, has_side_effects=True, vmem_limit_bytes=67_000_000
        ),
    )(
        video, emb, cond_weight, spatial_gain[None], spatial_qkv, spatial_out,
        temporal_gain[None], temporal_qkv, temporal_out, merge_weight, coarse_gain[None],
        coarse_qkv, coarse_out, up_weight,
    )
    return pl.pallas_call(
        combine,
        name="combine",
        out_shape=jax.ShapeDtypeStruct(video.shape, BF16),
        in_specs=[any_, any_],
        out_specs=any_,
        scratch_shapes=[
            b(4, GROUP, 16, D), b(512, 256), b(4, 512, D), b(256, 256), b(2, 256, 64),
            pltpu.SemaphoreType.DMA((9,)), pltpu.SemaphoreType.DMA((8,)),
        ],
    )(fine, coarse)


def solution(mesh):
    return jax.shard_map(
        body,
        mesh=mesh,
        in_specs=(P(("clip", "frame"), None, None), P("clip")) + (P(),) * 12,
        out_specs=P(("clip", "frame"), None, None),
        check_vma=False,
    )
```

```python
import math

import jax
import jax.numpy as jnp
from jax import lax
from jax.experimental import pallas as pl
from jax.experimental.pallas import tpu as pltpu
from jax.sharding import PartitionSpec as P

D = 512
DC = 1024
HEAD = 64
FREQ = 64
GROUP = 32
MESH = pl.DeviceIdType.MESH
F32 = jnp.float32
BF16 = jnp.bfloat16
QSCALE = math.log2(math.e) / math.sqrt(HEAD)

OFFSETS = sorted(
    [(a, b, d) for a in range(4) for b in range(4) for d in range(2) if (a, b, d) != (0, 0, 0)],
    key=lambda o: -(min(o[0], 4 - o[0]) + min(o[1], 4 - o[1]) + o[2]),
)


def dot(a, b):
    return jnp.dot(a, b, preferred_element_type=F32)


def dot_t(a, b):
    return lax.dot_general(a, b, (((1,), (1,)), ((), ())), preferred_element_type=F32)


def onehot(rows, columns, column_of):
    r = lax.broadcasted_iota(jnp.int32, (rows, columns), 0)
    c = lax.broadcasted_iota(jnp.int32, (rows, columns), 1)
    return jnp.where(c == column_of(r), 1.0, 0.0).astype(BF16)


def rms(x):
    return x * lax.rsqrt(jnp.mean(x * x, axis=-1, keepdims=True) + 1e-06)


def finish_pair(s, vst, ones, keys):
    s_lo, s_hi = s[:, :keys], s[:, keys:]
    p_lo = jnp.exp2(s_lo - jnp.max(s_lo, axis=-1, keepdims=True)).astype(BF16)
    p_hi = jnp.exp2(s_hi - jnp.max(s_hi, axis=-1, keepdims=True)).astype(BF16)
    p = jnp.concatenate([p_lo, p_hi], axis=1)
    o = dot(p, jnp.concatenate([vst, ones], axis=1))
    return (o[:, :128] / o[:, 128:]).astype(BF16)


def pipelined(blocks, scores, finish):
    ahead = scores(*blocks[0])
    for n, block in enumerate(blocks):
        now = ahead
        if n + 1 < len(blocks):
            ahead = scores(*blocks[n + 1])
        finish(now, *block)


def kernel(
    video, emb, cond, sgain, sqkv, sout, tgain, tqkv, tout, merge, cgain, cqkv, cout, up,
    recv2, zr,
    vid, wcond, wsq, wso, wtq, wto, wm, wcq, wco, wup,
    sq, skst, svst, ones_s, smix,
    sbuf1, recv1,
    perm, xt, tn, tq, tkst, tvst, ones_t, tmix,
    sbuf2, cbuf,
    c0, cq, ck, cv, cmix, zs,
    modv, lsem, vsem, osem, ss1, rs1, ss2, rs2, ss3, rs3,
):
    clip = lax.axis_index("clip")
    me = lax.axis_index("frame")
    z, x, y = me // 8, lax.rem(me // 2, 4), lax.rem(me, 2)

    def peer(o):
        return lax.rem(z + o[0], 4) * 8 + lax.rem(x + o[1], 4) * 2 + lax.rem(y + o[2], 2)

    barrier = pltpu.get_barrier_semaphore()
    for o in OFFSETS:
        pl.semaphore_signal(barrier, inc=1, device_id=(clip, peer(o)), device_id_type=MESH)

    weights = [
        (cond, wcond), (sqkv, wsq), (sout, wso), (tqkv, wtq), (tout, wto),
        (merge, wm), (cqkv, wcq), (cout, wco), (up, wup),
    ]
    wcopy = [pltpu.make_async_copy(a, b, lsem.at[i]) for i, (a, b) in enumerate(weights)]
    vcopy = [pltpu.make_async_copy(video.at[f], vid.at[f], vsem.at[f]) for f in range(4)]
    vcopy[0].start()
    for i in range(3):
        wcopy[i].start()
    for f in range(1, 4):
        vcopy[f].start()

    lane = lax.broadcasted_iota(jnp.int32, (1, 128), 1)
    lo = jnp.where(lane < HEAD, 1.0, 0.0).astype(F32)
    hi = 1.0 - lo
    ones_s[0:512, :] = jnp.broadcast_to(lo, (512, 128)).astype(BF16)
    ones_s[512:1024, :] = jnp.broadcast_to(hi, (512, 128)).astype(BF16)
    ones_t[0:128, :] = jnp.broadcast_to(lo, (128, 128)).astype(BF16)
    ones_t[128:256, :] = jnp.broadcast_to(hi, (128, 128)).astype(BF16)
    perm[...] = onehot(256, 256, lambda r: (r & 15) * 16 + (r >> 4))

    wcopy[0].wait()
    e1 = emb[...].astype(BF16).astype(F32)
    e2 = (emb[...] - e1).astype(BF16).astype(F32)
    e3 = emb[...] - e1 - e2
    piece = lax.broadcasted_iota(jnp.int32, (8, 128), 0)
    pieces = jnp.where(piece == 0, e1, jnp.where(piece == 1, e2, jnp.where(piece == 2, e3, 0.0)))
    modv[...] = jnp.sum(dot(pieces.astype(BF16), wcond[...]), axis=0, keepdims=True)
    sg = sgain[...] * (1.0 + modv[:, 0:D])
    shs = modv[:, D : 2 * D]
    tg = tgain[...] * (1.0 + modv[:, 2 * D : 3 * D])
    sht = modv[:, 3 * D : 4 * D]

    wcopy[1].wait()
    wcopy[2].wait()
    for i in range(3, 9):
        wcopy[i].start()

    def frame_step(f, carry):
        pltpu.make_async_copy(video.at[f], vid.at[f], vsem.at[f]).wait()
        xf = vid[f].astype(F32)
        normed = (rms(xf) * sg + shs).astype(BF16)
        sq[...] = (dot(normed, wsq[:, 0:D]) * QSCALE).astype(BF16)
        for p in range(4):
            k2 = dot(normed, wsq[:, D + p * 128 : D + (p + 1) * 128])
            skst[p, 0:512] = (k2 * lo).astype(BF16)
            skst[p, 512:1024] = (k2 * hi).astype(BF16)
            v2 = dot(normed, wsq[:, 2 * D + p * 128 : 2 * D + (p + 1) * 128])
            svst[p, 0:512] = (v2 * lo).astype(BF16)
            svst[p, 512:1024] = (v2 * hi).astype(BF16)

        @pl.when(f == 0)
        def _():
            pl.semaphore_wait(barrier, len(OFFSETS))

        def rows_of(dz):
            return pl.ds(pl.multiple_of(lax.rem(z + dz, 4) * 128, 128), 128)

        def scores(dz, p):
            return dot_t(sq[rows_of(dz), p * 128 : (p + 1) * 128], skst[p])

        def finish(v, dz, p):
            rows = rows_of(dz)
            smix[rows, p * 128 : (p + 1) * 128] = finish_pair(v, svst[p], ones_s[...], 512)
            if p < 3:
                return
            sbuf1[f, rows, :] = (vid[f, rows, :].astype(F32) + dot(smix[rows, :], wso[...])).astype(BF16)
            if dz == 0:
                own = pl.ds(pl.multiple_of(me * 16, 16), 16)
                recv1[f * GROUP + me] = sbuf1[f, own, :]
            for o in OFFSETS:
                if o[0] == dz:
                    to = peer(o)
                    pltpu.make_async_remote_copy(
                        src_ref=sbuf1.at[f, pl.ds(pl.multiple_of(to * 16, 16), 16), :],
                        dst_ref=recv1.at[f * GROUP + me],
                        send_sem=ss1,
                        recv_sem=rs1.at[f],
                        device_id=(clip, to),
                        device_id_type=MESH,
                    ).start()

        pipelined([(dz, p) for dz in (2, 1, 3, 0) for p in range(4)], scores, finish)
        return carry

    lax.fori_loop(0, 4, frame_step, 0)

    wcopy[3].wait()
    wcopy[4].wait()

    def group_step(j, carry):
        pltpu.make_async_copy(recv1.at[pl.ds(0, 31)], recv1.at[pl.ds(0, 31)], rs1.at[j]).wait()
        for sb in range(2):
            base = j * GROUP + sb * 16
            frames = pl.ds(pl.multiple_of(base, 16), 16)
            yg = dot(perm[...], recv1[frames].reshape(256, D))
            xt[:, frames, :] = yg.astype(BF16).reshape(16, 16, D)
            tn[:, frames, :] = (rms(yg) * tg + sht).astype(BF16).reshape(16, 16, D)
        return carry

    lax.fori_loop(0, 4, group_step, 0)

    def token_step(c, carry):
        normed = tn[pl.ds(c * 4, 4)].reshape(512, D)
        tq[...] = (dot(normed, wtq[:, 0:D]) * QSCALE).astype(BF16).reshape(4, 128, D)
        for p in range(4):
            k2 = dot(normed, wtq[:, D + p * 128 : D + (p + 1) * 128])
            tkst[:, p, 0:128, :] = (k2 * lo).astype(BF16).reshape(4, 128, 128)
            tkst[:, p, 128:256, :] = (k2 * hi).astype(BF16).reshape(4, 128, 128)
            v2 = dot(normed, wtq[:, 2 * D + p * 128 : 2 * D + (p + 1) * 128])
            tvst[:, p, 0:128, :] = (v2 * lo).astype(BF16).reshape(4, 128, 128)
            tvst[:, p, 128:256, :] = (v2 * hi).astype(BF16).reshape(4, 128, 128)

        def scores(q, p):
            return dot_t(tq[q, :, p * 128 : (p + 1) * 128], tkst[q, p])

        def finish(v, q, p):
            tmix[q, :, p * 128 : (p + 1) * 128] = finish_pair(
                v, tvst[q, p], ones_t[...], 128
            )

        pipelined([(q, p) for q in range(4) for p in range(4)], scores, finish)
        for q in range(4):
            tmix[q] = (xt[c * 4 + q].astype(F32) + dot(tmix[q], wto[...])).astype(BF16)
        for sb in range(2):
            fg = jnp.concatenate(
                [
                    tmix[q, j * GROUP + sb * 16 : j * GROUP + (sb + 1) * 16, :]
                    for j in range(4) for q in range(4)
                ],
                axis=0,
            )
            sbuf2[c, sb * 16 : (sb + 1) * 16] = dot(perm[...], fg).astype(BF16).reshape(16, 16, D)
        pltpu.make_async_copy(sbuf2.at[c, me], recv2.at[c, me], osem.at[c]).start()
        for o in OFFSETS:
            to = peer(o)
            pltpu.make_async_remote_copy(
                src_ref=sbuf2.at[c, to],
                dst_ref=recv2.at[c, me],
                send_sem=ss2,
                recv_sem=rs2,
                device_id=(clip, to),
                device_id_type=MESH,
            ).start()
        for d in range(2):
            for q in range(4):
                for jh in range(2):
                    j = 2 * jh + d
                    cbuf[
                        pl.ds(pl.multiple_of(c * 64 + jh * 32, 32), 32),
                        (d * 4 + q) * D : (d * 4 + q + 1) * D,
                    ] = tmix[q, j * GROUP : (j + 1) * GROUP, :]
        return carry

    lax.fori_loop(0, 4, token_step, 0)
    mine = pl.ds(pl.multiple_of(me * 16, 16), 16)

    for i in range(5, 9):
        wcopy[i].wait()
    c0[...] = dot(cbuf[...], wm[...]).astype(BF16)
    normed = (rms(c0[...].astype(F32)) * cgain[...]).astype(BF16)
    cq[...] = (dot(normed, wcq[:, 0:DC]) * QSCALE).astype(BF16)
    ck[...] = dot(normed, wcq[:, DC : 2 * DC]).astype(BF16)
    cv[...] = dot(normed, wcq[:, 2 * DC : 3 * DC]).astype(BF16)
    lane4 = lax.broadcasted_iota(jnp.int32, (64, 256), 1) >> 6
    block4 = jnp.concatenate(
        [jnp.where(lane4 == h, 1.0, 0.0).astype(BF16) for h in range(4)], axis=0
    )
    low = lax.broadcasted_iota(jnp.int32, (64, 128), 1) < HEAD

    def cell_scores(b, hg):
        rows, lanes = slice(b * 64, (b + 1) * 64), slice(hg * 256, (hg + 1) * 256)
        return dot_t(cq[rows, lanes], jnp.concatenate([ck[rows, lanes]] * 4, axis=0) * block4)

    def cell_finish(s, b, hg):
        rows, lanes = slice(b * 64, (b + 1) * 64), slice(hg * 256, (hg + 1) * 256)
        parts = []
        for half in range(2):
            sh = s[:, half * 128 : (half + 1) * 128]
            m_lo = jnp.max(jnp.where(low, sh, -jnp.inf), axis=-1, keepdims=True)
            m_hi = jnp.max(jnp.where(low, -jnp.inf, sh), axis=-1, keepdims=True)
            parts.append(jnp.exp2(sh - jnp.where(low, m_lo, m_hi)).astype(BF16))
        p = jnp.concatenate(parts, axis=1)
        o = dot(p, jnp.concatenate([cv[rows, lanes]] * 4, axis=0) * block4)
        cmix[rows, lanes] = (o / dot(p, block4)).astype(BF16)

    pipelined([(b, hg) for b in range(4) for hg in range(4)], cell_scores, cell_finish)
    coarse1 = (c0[...].astype(F32) + dot(cmix[...], wco[...])).astype(BF16)
    upped = dot(coarse1, wup[...]).astype(BF16)

    def pick(half):
        r = lax.broadcasted_iota(jnp.int32, (512, 256), 0)
        c = lax.broadcasted_iota(jnp.int32, (512, 256), 1)
        hit = (c == (r & 3) * 64 + ((r >> 2) & 1) * 32 + (r >> 4)) & (((r >> 3) & 1) == half)
        return jnp.where(hit, 1.0, 0.0).astype(BF16)

    zs[...] = (dot(pick(0), upped[:, :256]) + dot(pick(1), upped[:, 256:])).astype(BF16)
    own_z = pltpu.make_async_copy(zs.at[mine], zr.at[mine], osem.at[4])
    own_z.start()
    for o in OFFSETS:
        to = peer(o)
        pltpu.make_async_remote_copy(
            src_ref=zs.at[pl.ds(pl.multiple_of(to * 16, 16), 16), :],
            dst_ref=zr.at[mine, :],
            send_sem=ss3,
            recv_sem=rs3,
            device_id=(clip, to),
            device_id_type=MESH,
        ).start()

    pltpu.make_async_copy(recv2.at[:, pl.ds(0, 31)], recv2.at[:, pl.ds(0, 31)], rs2).wait()
    pltpu.make_async_copy(zr.at[pl.ds(0, 496)], zr.at[pl.ds(0, 496)], rs3).wait()
    pltpu.make_async_copy(sbuf1.at[:, pl.ds(0, 496), :], sbuf1.at[:, pl.ds(0, 496), :], ss1).wait()
    pltpu.make_async_copy(sbuf2.at[:, pl.ds(0, 31)], sbuf2.at[:, pl.ds(0, 31)], ss2).wait()
    pltpu.make_async_copy(zs.at[pl.ds(0, 496)], zs.at[pl.ds(0, 496)], ss3).wait()
    for c in range(4):
        pltpu.make_async_copy(sbuf2.at[c, me], recv2.at[c, me], osem.at[c]).wait()
    own_z.wait()


def combine(fine, coarse, out, got, zin, res, perm, spread, isem, osem):
    def part(sb):
        return pl.ds(sb * 4, 4)

    zcopy = pltpu.make_async_copy(coarse, zin, isem.at[8])
    zcopy.start()
    icopy = [
        pltpu.make_async_copy(fine.at[:, part(sb)], got.at[:, part(sb)], isem.at[sb])
        for sb in range(8)
    ]
    for cp in icopy:
        cp.start()
    perm[...] = onehot(
        256, 256, lambda r: ((r >> 2) & 3) * 64 + ((r >> 4) & 3) * 16 + (r >> 6) * 4 + (r & 3)
    )
    for half in range(2):
        spread[half] = onehot(
            256, 64,
            lambda r: ((r >> 4) & 3) * 16 + half * 8 + (r >> 7) * 4 + ((r >> 2) & 3),
        )
    zcopy.wait()
    ocopy = []
    for sb in range(8):
        icopy[sb].wait()
        rows = slice(sb * 64, (sb + 1) * 64)
        cells = jnp.concatenate([got[c, part(sb)].reshape(64, D) for c in range(4)], axis=0)
        for half in range(2):
            lanes = slice(half * 256, (half + 1) * 256)
            total = dot(perm[...], cells[:, lanes]) + dot(spread[half], zin[rows, :])
            for j in range(4):
                res[j, rows, lanes] = total[j * 64 : (j + 1) * 64].astype(BF16)
        cp = pltpu.make_async_copy(
            res.at[:, pl.ds(sb * 64, 64), :], out.at[:, pl.ds(sb * 64, 64), :], osem.at[sb]
        )
        cp.start()
        ocopy.append(cp)
    for cp in ocopy:
        cp.wait()


def body(
    video, timestep, cond_weight, spatial_gain, spatial_qkv, spatial_out, temporal_gain,
    temporal_qkv, temporal_out, merge_weight, coarse_gain, coarse_qkv, coarse_out, up_weight,
):
    counter = jnp.arange(FREQ, dtype=F32)
    frequency = jnp.exp(counter * (-math.log(10000.0) / FREQ))
    angles = timestep.astype(F32)[0] * frequency
    emb = jnp.concatenate([jnp.sin(angles), jnp.cos(angles)])[None]
    any_, vm = pl.BlockSpec(memory_space=pl.ANY), pl.BlockSpec(memory_space=pltpu.VMEM)
    b = lambda *shape: pltpu.VMEM(shape, BF16)
    fine, coarse = pl.pallas_call(
        kernel,
        name="denoise",
        out_shape=[
            jax.ShapeDtypeStruct((4, GROUP, 16, D), BF16),
            jax.ShapeDtypeStruct((512, 256), BF16),
        ],
        in_specs=[any_, vm, any_, vm, any_, any_, vm, any_, any_, any_, vm, any_, any_, any_],
        out_specs=[any_, any_],
        scratch_shapes=[
            b(4, 512, D), b(128, 2048), b(D, 3 * D), b(D, D), b(D, 3 * D), b(D, D),
            b(8 * D, DC), b(DC, 3 * DC), b(DC, DC), b(DC, D),
            b(512, D), b(4, 1024, 128), b(4, 1024, 128), b(1024, 128), b(512, D),
            b(4, 512, D), b(128, 16, D),
            b(256, 256), b(16, 128, D), b(16, 128, D), b(4, 128, D), b(4, 4, 256, 128),
            b(4, 4, 256, 128), b(256, 128), b(4, 128, D),
            b(4, 32, 16, D), b(256, 8 * D),
            b(256, DC), b(256, DC), b(256, DC), b(256, DC), b(256, DC), b(512, 256),
            pltpu.VMEM((1, 4 * D), F32),
            pltpu.SemaphoreType.DMA((9,)), pltpu.SemaphoreType.DMA((4,)),
            pltpu.SemaphoreType.DMA((8,)),
            pltpu.SemaphoreType.DMA, pltpu.SemaphoreType.DMA((4,)),
        ] + [pltpu.SemaphoreType.DMA] * 4,
        compiler_params=pltpu.CompilerParams(
            collective_id=0, has_side_effects=True, vmem_limit_bytes=67_000_000
        ),
    )(
        video, emb, cond_weight, spatial_gain[None], spatial_qkv, spatial_out,
        temporal_gain[None], temporal_qkv, temporal_out, merge_weight, coarse_gain[None],
        coarse_qkv, coarse_out, up_weight,
    )
    return pl.pallas_call(
        combine,
        name="combine",
        out_shape=jax.ShapeDtypeStruct(video.shape, BF16),
        in_specs=[any_, any_],
        out_specs=any_,
        scratch_shapes=[
            b(4, GROUP, 16, D), b(512, 256), b(4, 512, D), b(256, 256), b(2, 256, 64),
            pltpu.SemaphoreType.DMA((9,)), pltpu.SemaphoreType.DMA((8,)),
        ],
    )(fine, coarse)


def solution(mesh):
    return jax.shard_map(
        body,
        mesh=mesh,
        in_specs=(P(("clip", "frame"), None, None), P("clip")) + (P(),) * 12,
        out_specs=P(("clip", "frame"), None, None),
        check_vma=False,
    )
```
